32 devices in a mesh: expert: 8 (over y, x, core), row: 4 (over z).
Axes of the slice: x: 2, y: 2, z: 4, core: 2. Of those that a mesh axis runs over, the one named last changes fastest.
Arguments:
- weights: bfloat16 [8, 7168, 2048], P('expert', 'row'), may hold values from -6 to 6
- left_bits: int32 [8, 7168], P('expert', 'row'), may hold values from 0 to 1
- right_bits: int32 [8, 2048], P('expert'), may hold values from 0 to 1
- groups: int32 [8, 2048], P('expert'), may hold values from 0 to 15, never falling along the last dimension, each value on 1 to 256 neighbouring positions
Outputs:
- scaled: bfloat16 [8, 7168, 2048], P('expert', 'row')
- block_error: float32 [8, 7168, 256], P('expert', 'row')
- scales: float32 [8, 16], P('expert')
- expert_error: float32 [8], P('expert')
- total_error: float32 [], replicated
The draws below stay inside these ranges and needn't reach their ends.
Inputs may be any that keep to these rules, and one draw needn't show every extreme that they name: Along each expert's 2048 columns the group number never falls; each of the 16 groups holds 1 to 256 columns.
All inputs are finite; a program needn't handle non-finite values.
Results may differ from the reference program's by a relative error of at most 0.0091.
Values may be sent and summed in bfloat16 or wider, within the bound.
No kernel may reach another device: no remote copies, remote signals or barrier semaphores. Data moves between devices by JAX's collectives and lax.ppermute only.
A program may use at most 192 MiB of HBM per device.

```python
import math
import jax
import jax.numpy as jnp
import numpy as np
from jax import lax

D = 7168
FF = 2048
HB = 128
OUTER = 16
GROUPS = 16
BLOCKS = 56
GROUP_MOST = 256
EXPERTS = 8


def draw_weights(key, part):
    scale_key = jax.random.fold_in(key, 11)
    entry_key = jax.random.fold_in(key, 12)
    magnitude = jnp.exp(jax.random.uniform(scale_key, (EXPERTS, 1, 1), jnp.float32, math.log(0.02), math.log(1.0)))
    entries = jnp.clip(jax.random.normal(entry_key, (EXPERTS, D, FF), jnp.float32), -6.0, 6.0)
    return jnp.clip(entries * magnitude, -6.0, 6.0).astype(jnp.bfloat16)


def place_ends(result, stream_key, low, high):
    longest = result.shape.index(max(result.shape))
    spots = []
    for shift in (0, 1):
        where = [jax.random.randint(jax.random.fold_in(stream_key, axis), (), 0, length) for axis, length in enumerate(result.shape)]
        where[longest] = (where[longest] + shift) % result.shape[longest]
        spots.append(tuple(where))
    return result.at[spots[0]].set(low).at[spots[1]].set(high)


def profile(number_of, total, most, slope):
    loads = [(1 << 20) // math.isqrt(grade ** slope) + 1 for grade in range(2, number_of + 1)]
    spare, holding = total - most - (number_of - 1), [1] * (number_of - 1)
    while spare > 0:
        free = [i for i in range(number_of - 1) if holding[i] < most]
        whole, left = sum([loads[i] for i in free]), spare
        for i in free:
            more = min(most - holding[i], max(1, left * loads[i] // whole), spare)
            holding[i] = holding[i] + more
            spare = spare - more
    return np.array([most] + holding)


def ragged(key, amount, total, bound, skew):
    if amount == 2:
        one = jax.random.randint(key, (), max(1, total - bound), min(bound, total - 1) + 1)
        return jnp.stack([one, total - one])
    lengths = jnp.asarray(profile(amount, total, bound, skew), jnp.int32)
    couples = (amount - 1) // 2
    donor, receiver = lengths[1:1 + 2 * couples:2], lengths[2:2 + 2 * couples:2]
    room = jnp.minimum(donor - 1, bound - receiver)
    passed = jax.random.randint(jax.random.fold_in(key, 1), (couples,), 0, 1 << 20) % (room + 1)
    lengths = lengths.at[1:1 + 2 * couples:2].set(donor - passed).at[2:2 + 2 * couples:2].set(receiver + passed)
    return lengths[jax.random.permutation(jax.random.fold_in(key, 2), amount)]


def setup_inputs(seed: int = 0) -> dict:
    streams_of = jax.random.split(jax.random.key(seed), 5)
    return {
        "weights": draw_weights(jax.random.fold_in(streams_of[4], 71), 0),
        "left_bits": place_ends(jax.random.randint(streams_of[1], (EXPERTS, D), 0, 2), jax.random.fold_in(streams_of[1], 1), 0, 1).astype(jnp.int32),
        "right_bits": place_ends(jax.random.randint(streams_of[2], (EXPERTS, FF), 0, 2), jax.random.fold_in(streams_of[2], 1), 0, 1).astype(jnp.int32),
        "groups": jax.vmap(lambda own: jnp.searchsorted(jnp.cumsum(ragged(own, GROUPS, FF, GROUP_MOST, 1)), jnp.arange(FF), side="right"))(jax.random.split(streams_of[3], EXPERTS)).reshape((EXPERTS, FF)).astype(jnp.int32),
    }


def sylvester(order):
    row_index = jnp.arange(order, dtype=jnp.int32)[:, None]
    col_index = jnp.arange(order, dtype=jnp.int32)[None, :]
    common = jnp.bitwise_and(row_index, col_index)
    parity = jnp.zeros((order, order), jnp.int32)
    for bit_pos in range(order.bit_length() - 1):
        parity = parity + jnp.bitwise_and(jnp.right_shift(common, bit_pos), 1)
    return (1 - 2 * jnp.bitwise_and(parity, 1)).astype(jnp.float32)

def cosine_block(order):
    first = jnp.arange(order, dtype=jnp.float32)[:, None]
    second = jnp.arange(order, dtype=jnp.float32)[None, :]
    table = math.sqrt(2.0 / order) * jnp.cos(math.pi * (2.0 * second + 1.0) * first / (2.0 * order))
    return jnp.where(first == 0.0, table * math.sqrt(0.5), table)

def coset_error(values):
    nearest = jnp.floor(values + 0.5)
    offset = values - nearest
    squares = lax.optimization_barrier(jnp.sum(offset * offset, axis=-1))
    largest = lax.optimization_barrier(jnp.max(jnp.abs(offset), axis=-1))
    parity = jnp.mod(lax.optimization_barrier(jnp.sum(nearest, axis=-1)), 2.0)
    return jnp.where(parity > 0.5, squares + 1.0 - 2.0 * largest, squares)

def lattice_error(values):
    octets = values.reshape(values.shape[:-1] + (values.shape[-1] // 8, 8))
    return jnp.minimum(coset_error(octets), coset_error(octets - 0.5))

def reference(weights, left_bits, right_bits, groups):
    column_hadamard = sylvester(FF // OUTER)
    outer_hadamard = sylvester(OUTER)
    row_hadamard = sylvester(HB)
    block_matrix = cosine_block(BLOCKS).astype(jnp.bfloat16).astype(jnp.float32)
    group_ids = jnp.arange(GROUPS, dtype=jnp.int32)
    row_weight = (1.0 + 4.0 * (jnp.arange(D, dtype=jnp.float32) + 0.5) / D) / 3.0
    high = lax.Precision.HIGHEST

    def one_expert(operands):
        weight, left, right, group = operands
        left_sign = (2 * left - 1).astype(jnp.float32)
        right_sign = (2 * right - 1).astype(jnp.float32)
        signed = (weight.astype(jnp.float32) * left_sign[:, None] * right_sign[None, :]).astype(jnp.bfloat16)
        shaped = signed.astype(jnp.float32).reshape(D, OUTER, FF // OUTER)
        inner = jnp.einsum('dpq,qs->dps', shaped, column_hadamard, precision=high)
        outer = jnp.einsum('dps,pt->dts', inner, outer_hadamard, precision=high)
        columns = (outer.reshape(D, FF) / math.sqrt(FF)).astype(jnp.bfloat16)
        blocked = columns.astype(jnp.float32).reshape(BLOCKS, HB, FF)
        mixed_rows = jnp.einsum('ij,jbf->ibf', block_matrix, blocked, precision=high)
        rotated = jnp.einsum('ibf,bk->ikf', mixed_rows, row_hadamard, precision=high) / math.sqrt(HB)
        rotated = rotated.reshape(D, FF)
        column_peak = lax.optimization_barrier(jnp.max(jnp.abs(rotated), axis=0))
        in_group = group[None, :] == group_ids[:, None]
        group_peak = jnp.maximum(lax.optimization_barrier(jnp.max(jnp.where(in_group, column_peak[None, :], 0.0), axis=1)), 1.0)
        column_scale = lax.optimization_barrier(jnp.sum(jnp.where(in_group, (2.0 / group_peak)[:, None], 0.0), axis=0))
        values = rotated * column_scale[None, :]
        block_errors = lattice_error(values)
        mean_error = jnp.sum(block_errors * row_weight[:, None]) / (D * FF // 8)
        return (values.astype(jnp.bfloat16), block_errors, group_peak / 2.0, mean_error)
    scaled, block_error, scales, expert_error = lax.map(one_expert, (weights, left_bits, right_bits, groups))
    total_error = jnp.mean(expert_error)
    return (scaled, block_error, scales, expert_error, total_error)
```

```python
import math

import jax
import jax.numpy as jnp
from jax import lax
from jax.experimental import pallas as pl
from jax.experimental.pallas import tpu as pltpu
from jax.sharding import PartitionSpec as P

HB = 128
GROUPS = 16
INNER = 256
LOW = 16
CHUNKS = 2
OCTET = 8


def sylvester(order):
    row_index = jnp.arange(order, dtype=jnp.int32)[:, None]
    col_index = jnp.arange(order, dtype=jnp.int32)[None, :]
    common = jnp.bitwise_and(row_index, col_index)
    parity = jnp.zeros((order, order), jnp.int32)
    for bit_pos in range(order.bit_length() - 1):
        parity = parity + jnp.bitwise_and(jnp.right_shift(common, bit_pos), 1)
    return (1 - 2 * jnp.bitwise_and(parity, 1)).astype(jnp.float32)


def cosine_entries(first, second, order):
    first = first.astype(jnp.float32)[:, None]
    second = second.astype(jnp.float32)[None, :]
    table = math.sqrt(2.0 / order) * jnp.cos(math.pi * (2.0 * second + 1.0) * first / (2.0 * order))
    return jnp.where(first == 0.0, table * math.sqrt(0.5), table)


def butterfly(parts):
    parts = list(parts)
    step = 1
    while step < len(parts):
        for base in range(len(parts)):
            if not base & step:
                low, high = parts[base], parts[base | step]
                parts[base], parts[base | step] = low + high, low - high
        step *= 2
    return parts


def column_transform(weights, left_bits, right_sign, inner_hadamard, place, ring):
    rows, width = weights.shape
    tile = HB
    piece = width // (CHUNKS * ring)
    root = 1.0 / math.sqrt(width)

    def kernel(place_ref, w_ref, left_ref, right_ref, h_ref, *rest):
        outs, stage = rest[:-1], rest[-1]
        mine = place_ref[0]
        eye_row = lax.broadcasted_iota(jnp.int32, (tile, tile), 0)
        eye_col = lax.broadcasted_iota(jnp.int32, (tile, tile), 1)
        signs = (2 * left_ref[...] - 1).astype(jnp.float32) * root
        left = jnp.sum(jnp.where(eye_row == eye_col, signs, 0.0), axis=1, keepdims=True)
        parts = []
        for hi in range(width // INNER):
            cols = slice(hi * INNER, (hi + 1) * INNER)
            signed = w_ref[:, cols] * right_ref[:, cols]
            parts.append(jnp.dot(signed, h_ref[...], preferred_element_type=jnp.float32))
        for hi, part in enumerate(butterfly(parts)):
            stage[:, hi * INNER : (hi + 1) * INNER] = (part * left).astype(jnp.bfloat16)
        for chunk in range(CHUNKS):
            for shift in range(ring):
                dest = lax.rem(mine + shift, ring)
                start = pl.multiple_of((chunk * ring + dest) * piece, 128)
                outs[chunk * ring + shift][...] = stage[:, pl.ds(start, piece)]

    pieces = CHUNKS * ring
    outs = pl.pallas_call(
        kernel,
        grid=(rows // tile,),
        in_specs=[
            pl.BlockSpec(memory_space=pltpu.SMEM),
            pl.BlockSpec((tile, width), lambda r: (r, 0)),
            pl.BlockSpec((1, tile), lambda r: (0, r)),
            pl.BlockSpec((1, width), lambda r: (0, 0)),
            pl.BlockSpec((INNER, INNER), lambda r: (0, 0)),
        ],
        out_specs=[pl.BlockSpec((tile, piece), lambda r: (r, 0))] * pieces,
        out_shape=[jax.ShapeDtypeStruct((rows, piece), jnp.bfloat16)] * pieces,
        scratch_shapes=[pltpu.VMEM((tile, width), jnp.bfloat16)],
        name="column_transform",
    )(place, weights, left_bits, right_sign, inner_hadamard)
    return [outs[c * ring : (c + 1) * ring] for c in range(CHUNKS)]


def row_mix(pieces, mixer):
    ring = len(pieces)
    rows, width = pieces[0].shape
    blocks = rows // HB
    high = HB // LOW
    band = blocks * LOW
    root = 1.0 / math.sqrt(HB)

    def kernel(*refs):
        ins, m_ref = refs[:ring], refs[ring]
        outs, peak_ref, stage = refs[ring + 1 : 2 * ring + 1], refs[2 * ring + 1], refs[2 * ring + 2]
        for hi in range(high):
            rhs = jnp.concatenate([r[:, hi].reshape(band, width) for r in ins], axis=0)
            stage[hi] = jnp.dot(m_ref[...], rhs, preferred_element_type=jnp.float32)

        peak_ref[...] = jnp.zeros_like(peak_ref)
        for shift in range(ring):

            def one(a, peak):
                start = pl.multiple_of(shift * band + a * LOW, LOW)
                parts = butterfly([stage[hi, pl.ds(start, LOW), :] for hi in range(high)])
                for hi, part in enumerate(parts):
                    part = part * root
                    peak = jnp.maximum(peak, jnp.abs(part))
                    outs[shift][a, hi] = part.astype(jnp.bfloat16)
                return peak

            peak = lax.fori_loop(0, blocks, one, jnp.zeros((LOW, width), jnp.float32))
            peak_ref[...] = jnp.maximum(peak_ref[...], jnp.max(peak, axis=0, keepdims=True))

    shaped = [p.reshape(blocks, high, LOW, width) for p in pieces]
    result = pl.pallas_call(
        kernel,
        out_shape=[jax.ShapeDtypeStruct((blocks, high, LOW, width), jnp.bfloat16)] * ring
        + [jax.ShapeDtypeStruct((1, width), jnp.float32)],
        scratch_shapes=[pltpu.VMEM((high, ring * band, width), jnp.float32)],
        name="row_mix",
    )(*shaped, mixer)
    return [y.reshape(rows, width) for y in result[:ring]], result[ring]


def quantize(chunk, pieces, scale_row, scale_octet, spread, numbers, before):
    ring = len(pieces)
    rows, piece = pieces[0].shape
    width = ring * piece
    lanes = width // OCTET
    tile = HB

    def kernel(num_ref, *refs):
        ins = refs[:ring]
        row_ref, oct_ref, spread_ref = refs[ring : ring + 3]
        scaled_ref, error_ref, sum_ref = refs[-3:]
        mine, first, total = num_ref[0], num_ref[1], num_ref[2]
        step = pl.program_id(0)
        held = [r[...] for r in ins]
        for shift in range(ring):
            start = pl.multiple_of(lax.rem(mine - shift + ring, ring) * piece, 128)
            scale = row_ref[:, pl.ds(start, piece)]
            scaled_ref[:, pl.ds(start, piece)] = (held[shift].astype(jnp.float32) * scale).astype(jnp.bfloat16)
        turned = jnp.dot(jnp.concatenate(held, axis=1), spread_ref[...], preferred_element_type=jnp.float32)
        near_sum = low_sum = squares = far_squares = largest = smallest = None
        for i in range(OCTET):
            value = turned[:, i * lanes : (i + 1) * lanes] * oct_ref[i : i + 1, :]
            near = jnp.floor(value + 0.5)
            low = jnp.floor(value)
            gap = jnp.abs(value - near)
            far = 0.5 - gap
            if i == 0:
                near_sum, low_sum, squares, far_squares = near, low, gap * gap, far * far
                largest = smallest = gap
            else:
                near_sum, low_sum = near_sum + near, low_sum + low
                squares, far_squares = squares + gap * gap, far_squares + far * far
                largest, smallest = jnp.maximum(largest, gap), jnp.minimum(smallest, gap)
        near_half, low_half = near_sum * 0.5, low_sum * 0.5
        whole = jnp.where(near_half != jnp.floor(near_half), squares + (1.0 - 2.0 * largest), squares)
        shifted = jnp.where(low_half != jnp.floor(low_half), far_squares + 2.0 * smallest, far_squares)
        error = jnp.minimum(whole, shifted)
        error_ref[...] = error
        position = lax.broadcasted_iota(jnp.int32, (tile, lanes), 0) + (first + step * tile)
        weight = (1.0 + 4.0 * (position.astype(jnp.float32) + 0.5) / total.astype(jnp.float32)) / 3.0
        part = jnp.sum((error * weight).reshape(tile // 8, 8, lanes), axis=0)

        @pl.when(step == 0)
        def _():
            sum_ref[...] = jnp.zeros_like(sum_ref)

        sum_ref[...] += part

    in_specs = [pl.BlockSpec(memory_space=pltpu.SMEM)]
    in_specs += [pl.BlockSpec((tile, piece), lambda r: (r, 0))] * ring
    in_specs += [
        pl.BlockSpec((1, width), lambda r: (0, chunk)),
        pl.BlockSpec((OCTET, lanes), lambda r: (0, chunk)),
        pl.BlockSpec((width, width), lambda r: (0, 0)),
    ]
    operands = [numbers, *pieces, scale_row, scale_octet, spread]
    aliases = {}
    if before is not None:
        aliases = {len(operands): 0, len(operands) + 1: 1}
        in_specs += [pl.BlockSpec(memory_space=pl.ANY)] * 2
        operands += list(before)
    return pl.pallas_call(
        kernel,
        grid=(rows // tile,),
        in_specs=in_specs,
        out_specs=[
            pl.BlockSpec((tile, width), lambda r: (r, chunk)),
            pl.BlockSpec((tile, lanes), lambda r: (r, chunk)),
            pl.BlockSpec((8, lanes), lambda r: (0, 0)),
        ],
        out_shape=[
            jax.ShapeDtypeStruct((rows, CHUNKS * width), jnp.bfloat16),
            jax.ShapeDtypeStruct((rows, CHUNKS * lanes), jnp.float32),
            jax.ShapeDtypeStruct((8, lanes), jnp.float32),
        ],
        input_output_aliases=aliases,
        name="quantize",
    )(*operands)


def mixer_table(mine, ring, blocks):
    local = jnp.arange(ring * blocks, dtype=jnp.int32)
    shift, inside = local // blocks, local % blocks
    to_row = ((mine + shift) % ring) * blocks + inside
    from_row = ((mine - shift + ring) % ring) * blocks + inside
    cosine = cosine_entries(to_row, from_row, ring * blocks).astype(jnp.bfloat16)
    side = ring * blocks * LOW
    table = cosine[:, None, :, None] * sylvester(LOW).astype(jnp.bfloat16)[None, :, None, :]
    return table.reshape(side, side)


def spread_table(mine, ring, piece):
    width = ring * piece
    row = jnp.arange(width, dtype=jnp.int32)
    natural = ((mine - row // piece + ring) % ring) * piece + row % piece
    target = (natural % OCTET) * (width // OCTET) + natural // OCTET
    return (target[:, None] == jnp.arange(width, dtype=jnp.int32)[None, :]).astype(jnp.bfloat16)


def body(weights, left_bits, right_bits, groups):
    experts, local_rows, width = weights.shape
    assert experts == 1
    ring = lax.axis_size("row")
    mine = lax.axis_index("row").astype(jnp.int32)
    blocks_here = local_rows // HB
    piece = width // (CHUNKS * ring)
    place = mine.reshape(1)

    def send(x, shift):
        return lax.ppermute(x, "row", [(k, (k + shift) % ring) for k in range(ring)])

    right_sign = (2 * right_bits - 1).astype(jnp.bfloat16)
    inner_hadamard = sylvester(INNER).astype(jnp.bfloat16)
    outgoing = column_transform(weights[0], left_bits, right_sign, inner_hadamard, place, ring)
    mixer = mixer_table(mine, ring, blocks_here)
    spread = spread_table(mine, ring, piece)
    returned, peaks = [], []
    for chunk in range(CHUNKS):
        held = [outgoing[chunk][0]] + [send(outgoing[chunk][s], s) for s in range(1, ring)]
        mixed, peak = row_mix(held, mixer)
        returned.append([mixed[0]] + [send(mixed[s], s) for s in range(1, ring)])
        peaks.append(peak)

    group_ids = jnp.arange(GROUPS, dtype=jnp.int32)[:, None]
    in_group = groups == group_ids
    own_groups = [
        lax.dynamic_slice_in_dim(groups, (chunk * ring + mine) * piece, piece, 1) for chunk in range(CHUNKS)
    ]
    own_in = jnp.concatenate(own_groups, axis=1) == group_ids
    partial_peak = jnp.max(jnp.where(own_in, jnp.concatenate(peaks, axis=1), 0.0), axis=1)
    group_peak = jnp.maximum(lax.pmax(partial_peak, "row"), 1.0)
    scale_row = jnp.sum(jnp.where(in_group, (2.0 / group_peak)[:, None], 0.0), axis=0)
    scale_octet = scale_row.reshape(width // OCTET, OCTET).T

    numbers = jnp.stack([mine, mine * local_rows, jnp.int32(local_rows) * ring])
    before, sums = None, []
    for chunk in range(CHUNKS):
        scaled, errors, part = quantize(
            chunk, returned[chunk], scale_row[None, :], scale_octet, spread, numbers, before
        )
        before = (scaled, errors)
        sums.append(jnp.sum(part))
    partial_error = sum(sums) / (local_rows * ring * width // OCTET)
    expert_count = experts * lax.axis_size("expert")
    expert = lax.axis_index("expert")
    slots = jnp.where(jnp.arange(expert_count) == expert, partial_error, 0.0)
    every_error = lax.psum(slots, ("expert", "row"))
    expert_error = lax.dynamic_slice_in_dim(every_error, expert, 1)
    total_error = jnp.sum(every_error) / expert_count
    return (scaled[None], errors[None], (group_peak / 2.0)[None], expert_error, total_error)


def solution(mesh):
    placed = (P("expert", "row", None), P("expert", "row"), P("expert", None), P("expert", None))
    return jax.shard_map(
        body,
        mesh=mesh,
        in_specs=placed,
        out_specs=(
            P("expert", "row", None),
            P("expert", "row", None),
            P("expert", None),
            P("expert"),
            P(),
        ),
        check_vma=False,
    )
```

```python
import math

import jax
import jax.numpy as jnp
from jax import lax
from jax.experimental import pallas as pl
from jax.experimental.pallas import tpu as pltpu
from jax.sharding import PartitionSpec as P

HB = 128
GROUPS = 16
INNER = 256
LOW = 16
CHUNKS = 4
AHEAD = 2
OCTET = 8


def butterfly(parts):
    parts = list(parts)
    step = 1
    while step < len(parts):
        for base in range(len(parts)):
            if not base & step:
                low, high = parts[base], parts[base | step]
                parts[base], parts[base | step] = low + high, low - high
        step *= 2
    return parts


def column_transform(weights, left_bits, right_bits, place, ring, chunks):
    rows, width = weights.shape
    tile = 2 * HB
    count = width // INNER
    piece = width // (chunks * ring)
    root = 1.0 / math.sqrt(width)

    def kernel(place_ref, w_ref, left_ref, right_ref, *rest):
        outs = rest[: chunks * ring]
        table, stage, left_col, natural = rest[chunks * ring :]
        mine = place_ref[0]

        @pl.when(pl.program_id(0) == 0)
        def _():
            common = lax.broadcasted_iota(jnp.int32, (INNER, INNER), 0) & lax.broadcasted_iota(
                jnp.int32, (INNER, INNER), 1
            )
            for bits in (4, 2, 1):
                common = common ^ (common >> bits)
            table[...] = (1 - 2 * (common & 1)).astype(jnp.float32).astype(jnp.bfloat16)

        eye = lax.broadcasted_iota(jnp.int32, (HB, HB), 0) == lax.broadcasted_iota(jnp.int32, (HB, HB), 1)
        for part in range(tile // HB):
            cols = slice(part * HB, (part + 1) * HB)
            signs = (2 * left_ref[:, cols] - 1).astype(jnp.float32) * root
            left_col[cols, :] = jnp.sum(jnp.where(eye, signs, 0.0), axis=1, keepdims=True)
        right = (2 * right_ref[...] - 1).astype(jnp.float32).astype(jnp.bfloat16)
        signed = [
            w_ref[:, hi * INNER : (hi + 1) * INNER] * right[:, hi * INNER : (hi + 1) * INNER]
            for hi in range(count)
        ]
        turned = jnp.dot(jnp.concatenate(signed, axis=0), table[...], preferred_element_type=jnp.float32)
        stage[...] = turned.reshape(count, tile, INNER)

        def one(group, _):
            start = pl.multiple_of(group * LOW, LOW)
            left = left_col[pl.ds(start, LOW), :]
            parts = butterfly([stage[hi, pl.ds(start, LOW), :] for hi in range(count)])
            for hi, part in enumerate(parts):
                natural[pl.ds(start, LOW), hi * INNER : (hi + 1) * INNER] = (part * left).astype(jnp.bfloat16)
            return 0

        lax.fori_loop(0, tile // LOW, one, 0)
        for chunk in range(chunks):
            for shift in range(ring):
                dest = lax.rem(mine + shift, ring)
                start = pl.multiple_of((chunk * ring + dest) * piece, 128)
                outs[chunk * ring + shift][...] = natural[:, pl.ds(start, piece)]

    pieces = chunks * ring
    outs = pl.pallas_call(
        kernel,
        grid=(rows // tile,),
        in_specs=[
            pl.BlockSpec(memory_space=pltpu.SMEM),
            pl.BlockSpec((tile, width), lambda r: (r, 0)),
            pl.BlockSpec((1, tile), lambda r: (0, r)),
            pl.BlockSpec((1, width), lambda r: (0, 0)),
        ],
        out_specs=[pl.BlockSpec((tile, piece), lambda r: (r, 0))] * pieces,
        out_shape=[jax.ShapeDtypeStruct((rows, piece), jnp.bfloat16)] * pieces,
        scratch_shapes=[
            pltpu.VMEM((INNER, INNER), jnp.bfloat16),
            pltpu.VMEM((count, tile, INNER), jnp.float32),
            pltpu.VMEM((tile, 1), jnp.float32),
            pltpu.VMEM((tile, width), jnp.bfloat16),
        ],
        name="column_transform",
    )(place, weights, left_bits, right_bits)
    return [outs[c * ring : (c + 1) * ring] for c in range(chunks)]


def row_mix(pieces, mixer, own_groups, before):
    ring = len(pieces)
    rows, width = pieces[0].shape
    blocks = rows // HB
    high = HB // LOW
    band = blocks * LOW
    root = 1.0 / math.sqrt(HB)

    def kernel(*refs):
        ins, m_ref, group_ref, before_ref = refs[:ring], refs[ring], refs[ring + 1], refs[ring + 2]
        outs, peak_ref, stage = refs[ring + 3 : 2 * ring + 3], refs[2 * ring + 3], refs[2 * ring + 4]
        for hi in range(high):
            rhs = jnp.concatenate([r[:, hi].reshape(band, width) for r in ins], axis=0)
            stage[hi] = jnp.dot(m_ref[...], rhs, preferred_element_type=jnp.float32)

        peak = jnp.zeros((LOW, width), jnp.float32)
        for shift in range(ring):

            def one(a, peak):
                start = pl.multiple_of(shift * band + a * LOW, LOW)
                parts = butterfly([stage[hi, pl.ds(start, LOW), :] for hi in range(high)])
                for hi, part in enumerate(parts):
                    part = part * root
                    peak = jnp.maximum(peak, jnp.abs(part))
                    outs[shift][a, hi] = part.astype(jnp.bfloat16)
                return peak

            peak = lax.fori_loop(0, blocks, one, peak)
        column_peak = jnp.max(peak, axis=0, keepdims=True)
        ids = lax.broadcasted_iota(jnp.int32, (GROUPS, width), 0)
        held = jnp.max(jnp.where(group_ref[...] == ids, column_peak, 0.0), axis=1, keepdims=True)
        peak_ref[...] = jnp.maximum(before_ref[...], held)

    shaped = [p.reshape(blocks, high, LOW, width) for p in pieces]
    result = pl.pallas_call(
        kernel,
        out_shape=[jax.ShapeDtypeStruct((blocks, high, LOW, width), jnp.bfloat16)] * ring
        + [jax.ShapeDtypeStruct((GROUPS, 128), jnp.float32)],
        scratch_shapes=[pltpu.VMEM((high, ring * band, width), jnp.float32)],
        name="row_mix",
    )(*shaped, mixer, own_groups, before)
    return [y.reshape(rows, width) for y in result[:ring]], result[ring]


def quantize(part_index, pieces, scale_row, scale_octet, spread, numbers, before):
    each = len(pieces)
    ring = len(pieces[0])
    rows, piece = pieces[0][0].shape
    width = each * ring * piece
    lanes = width // OCTET
    parts_in_all = scale_row.shape[1] // width
    tile = 2 * HB
    flat = [p for chunk in pieces for p in chunk]

    def kernel(num_ref, *refs):
        ins = refs[: each * ring]
        row_ref, oct_ref, spread_ref = refs[each * ring : each * ring + 3]
        scaled_ref, error_ref, sum_ref, stage = refs[-4:]
        mine, first, total = num_ref[0], num_ref[1], num_ref[2]
        step = pl.program_id(0)
        stage[...] = jnp.dot(
            jnp.concatenate([r[...] for r in ins], axis=1), spread_ref[...], preferred_element_type=jnp.float32
        )
        starts = []
        for index in range(each * ring):
            owner = lax.rem(mine - index % ring + ring, ring)
            starts.append(pl.multiple_of((index // ring * ring + owner) * piece, 128))
        share = 4.0 / (3.0 * total.astype(jnp.float32))

        def one(group, carry):
            held = pl.ds(pl.multiple_of(group * LOW, LOW), LOW)
            for index in range(each * ring):
                cols = pl.ds(starts[index], piece)
                scaled = ins[index][held, :].astype(jnp.float32) * row_ref[:, cols]
                scaled_ref[held, cols] = scaled.astype(jnp.bfloat16)
            near_sum = low_sum = squares = far_squares = largest = smallest = None
            for i in range(OCTET):
                value = stage[held, i * lanes : (i + 1) * lanes] * oct_ref[i : i + 1, :]
                near = jnp.floor(value + 0.5)
                low = jnp.floor(value)
                gap = jnp.abs(value - near)
                far = 0.5 - gap
                if i == 0:
                    near_sum, low_sum, squares, far_squares = near, low, gap * gap, far * far
                    largest = smallest = gap
                else:
                    near_sum, low_sum = near_sum + near, low_sum + low
                    squares, far_squares = squares + gap * gap, far_squares + far * far
                    largest, smallest = jnp.maximum(largest, gap), jnp.minimum(smallest, gap)
            near_half, low_half = near_sum * 0.5, low_sum * 0.5
            whole = jnp.where(near_half != jnp.floor(near_half), squares + (1.0 - 2.0 * largest), squares)
            shifted = jnp.where(low_half != jnp.floor(low_half), far_squares + 2.0 * smallest, far_squares)
            error = jnp.minimum(whole, shifted)
            error_ref[held, :] = error
            position = lax.broadcasted_iota(jnp.int32, (LOW, lanes), 0) + (first + step * tile + group * LOW)
            weight = (position.astype(jnp.float32) + 0.5) * share + (1.0 / 3.0)
            return carry + error * weight

        part = lax.fori_loop(0, tile // LOW, one, jnp.zeros((LOW, lanes), jnp.float32))

        @pl.when(step == 0)
        def _():
            sum_ref[...] = jnp.zeros_like(sum_ref)

        sum_ref[...] += part

    in_specs = [pl.BlockSpec(memory_space=pltpu.SMEM)]
    in_specs += [pl.BlockSpec((tile, piece), lambda r: (r, 0))] * (each * ring)
    in_specs += [
        pl.BlockSpec((1, width), lambda r: (0, part_index)),
        pl.BlockSpec((OCTET, lanes), lambda r: (0, part_index)),
        pl.BlockSpec((width, width), lambda r: (0, 0)),
    ]
    operands = [numbers, *flat, scale_row, scale_octet, spread]
    aliases = {}
    if before is not None:
        aliases = {len(operands): 0, len(operands) + 1: 1}
        in_specs += [pl.BlockSpec(memory_space=pl.ANY)] * 2
        operands += list(before)
    return pl.pallas_call(
        kernel,
        grid=(rows // tile,),
        in_specs=in_specs,
        out_specs=[
            pl.BlockSpec((tile, width), lambda r: (r, part_index)),
            pl.BlockSpec((tile, lanes), lambda r: (r, part_index)),
            pl.BlockSpec((LOW, lanes), lambda r: (0, 0)),
        ],
        out_shape=[
            jax.ShapeDtypeStruct((rows, parts_in_all * width), jnp.bfloat16),
            jax.ShapeDtypeStruct((rows, parts_in_all * lanes), jnp.float32),
            jax.ShapeDtypeStruct((LOW, lanes), jnp.float32),
        ],
        scratch_shapes=[pltpu.VMEM((tile, width), jnp.float32)],
        input_output_aliases=aliases,
        name="quantize",
    )(*operands)


def mixer_table(mine, ring, blocks):
    side = ring * blocks * LOW
    row = lax.broadcasted_iota(jnp.int32, (side, side), 0)
    col = lax.broadcasted_iota(jnp.int32, (side, side), 1)
    band = blocks * LOW
    first = (((mine + row // band) % ring) * blocks + (row % band) // LOW).astype(jnp.float32)
    second = (((mine - col // band + ring) % ring) * blocks + (col % band) // LOW).astype(jnp.float32)
    order = ring * blocks
    table = math.sqrt(2.0 / order) * jnp.cos(math.pi * (2.0 * second + 1.0) * first / (2.0 * order))
    table = jnp.where(first == 0.0, table * math.sqrt(0.5), table)
    common = (row % LOW) & (col % LOW)
    common = common ^ (common >> 2)
    common = common ^ (common >> 1)
    return jnp.where((common & 1) == 0, table, -table).astype(jnp.bfloat16)


def spread_table(mine, ring, piece, width):
    row = lax.broadcasted_iota(jnp.int32, (width, width), 0)
    col = lax.broadcasted_iota(jnp.int32, (width, width), 1)
    index = row // piece
    natural = (index // ring * ring + (mine - index % ring + ring) % ring) * piece + row % piece
    target = (natural % OCTET) * (width // OCTET) + natural // OCTET
    return (target == col).astype(jnp.bfloat16)


def body(weights, left_bits, right_bits, groups):
    experts, local_rows, width = weights.shape
    assert experts == 1
    ring = lax.axis_size("row")
    mine = lax.axis_index("row").astype(jnp.int32)
    blocks_here = local_rows // HB
    chunks = chunk_count(width, ring)
    piece = width // (chunks * ring)
    unit = OCTET * 128
    each = unit // (ring * piece)
    place = mine.reshape(1)

    def send(x, shift):
        return lax.ppermute(x, "row", [(k, (k + shift) % ring) for k in range(ring)])

    outgoing = column_transform(weights[0], left_bits, right_bits, place, ring, chunks)
    mixer = mixer_table(mine, ring, blocks_here)
    spread = spread_table(mine, ring, piece, unit)
    own_groups = [
        lax.dynamic_slice_in_dim(groups, (chunk * ring + mine) * piece, piece, 1) for chunk in range(chunks)
    ]
    received, returned = [], []
    peak = jnp.zeros((GROUPS, 128), jnp.float32)
    for chunk in range(chunks):
        leaving = outgoing[chunk][1:]
        if chunk >= AHEAD:
            leaving, received[chunk - AHEAD] = lax.optimization_barrier((leaving, received[chunk - AHEAD]))
        received.append([send(leaving[s - 1], s) for s in range(1, ring)])
    peaks = None
    for chunk in range(chunks):
        mixed, peak = row_mix([outgoing[chunk][0]] + received[chunk], mixer, own_groups[chunk], peak)
        if chunk == chunks - 1:
            peaks = [peak] + [send(peak, s) for s in range(1, ring)]
        returned.append([mixed[0]] + [send(mixed[s], s) for s in range(1, ring)])

    group_peak = jnp.max(jnp.stack(peaks), axis=(0, 2))
    group_peak = jnp.maximum(group_peak, 1.0)
    in_group = groups == jnp.arange(GROUPS, dtype=jnp.int32)[:, None]
    scale_row = jnp.sum(jnp.where(in_group, (2.0 / group_peak)[:, None], 0.0), axis=0)
    scale_octet = scale_row.reshape(width // OCTET, OCTET).T

    numbers = jnp.stack([mine, mine * local_rows, jnp.int32(local_rows) * ring])
    before, total = None, 0.0
    for part_index in range(width // unit):
        held = returned[part_index * each : (part_index + 1) * each]
        scaled, errors, part = quantize(
            part_index, held, scale_row[None, :], scale_octet, spread, numbers, before
        )
        before = (scaled, errors)
        total = total + part
    partial_error = jnp.sum(total) / (local_rows * ring * width // OCTET)
    expert_count = experts * lax.axis_size("expert")
    expert = lax.axis_index("expert")
    slots = jnp.where(jnp.arange(expert_count) == expert, partial_error, 0.0)
    every_error = lax.psum(slots, ("expert", "row"))
    expert_error = lax.dynamic_slice_in_dim(every_error, expert, 1)
    total_error = jnp.sum(every_error) / expert_count
    return (scaled[None], errors[None], (group_peak / 2.0)[None], expert_error, total_error)


def chunk_count(width, ring):
    return min(CHUNKS, width // (128 * ring))


def solution(mesh):
    placed = (P("expert", "row", None), P("expert", "row"), P("expert", None), P("expert", None))
    return jax.shard_map(
        body,
        mesh=mesh,
        in_specs=placed,
        out_specs=(
            P("expert", "row", None),
            P("expert", "row", None),
            P("expert", None),
            P("expert"),
            P(),
        ),
        check_vma=False,
    )
```

```python
import math

import jax
import jax.numpy as jnp
from jax import lax
from jax.experimental import pallas as pl
from jax.experimental.pallas import tpu as pltpu
from jax.sharding import PartitionSpec as P

HB = 128
GROUPS = 16
INNER = 256
LOW = 16
CHUNKS = 4
AHEAD = 2
OCTET = 8
TILE2 = 448


def butterfly(parts):
    parts = list(parts)
    step = 1
    while step < len(parts):
        for base in range(len(parts)):
            if not base & step:
                low, high = parts[base], parts[base | step]
                parts[base], parts[base | step] = low + high, low - high
        step *= 2
    return parts


def even_tile(rows, most):
    return max(t for t in range(HB, most + 1, HB // 2) if rows % t == 0)


def column_transform(weights, left_bits, right_bits, place, ring, chunks, first, rows, tile, before):
    all_rows, width = weights.shape
    skip = first // tile
    count = width // INNER
    piece = width // (chunks * ring)
    root = 1.0 / math.sqrt(width)

    def kernel(place_ref, w_ref, left_ref, right_ref, *rest):
        rest = rest[0 if before is None else len(before) :]
        outs = rest[: chunks * ring]
        table, stage, left_col = rest[chunks * ring :]
        mine = place_ref[0]

        @pl.when(pl.program_id(0) == 0)
        def _():
            common = lax.broadcasted_iota(jnp.int32, (INNER, INNER), 0) & lax.broadcasted_iota(
                jnp.int32, (INNER, INNER), 1
            )
            for bits in (4, 2, 1):
                common = common ^ (common >> bits)
            table[...] = (1 - 2 * (common & 1)).astype(jnp.float32).astype(jnp.bfloat16)

        eye = lax.broadcasted_iota(jnp.int32, (HB, HB), 0) == lax.broadcasted_iota(jnp.int32, (HB, HB), 1)
        for part in range(tile // HB):
            cols = slice(part * HB, (part + 1) * HB)
            signs = (2 * left_ref[:, cols] - 1).astype(jnp.float32) * root
            column = jnp.sum(jnp.where(eye, signs, 0.0), axis=1, keepdims=True)
            left_col[cols, :] = jnp.broadcast_to(column, (HB, INNER))
        right = (2 * right_ref[...] - 1).astype(jnp.float32).astype(jnp.bfloat16)
        signed = [
            w_ref[:, hi * INNER : (hi + 1) * INNER] * right[:, hi * INNER : (hi + 1) * INNER]
            for hi in range(count)
        ]
        turned = jnp.dot(jnp.concatenate(signed, axis=0), table[...], preferred_element_type=jnp.float32)
        stage[...] = turned.reshape(count, tile, INNER)

        def finish(here):
            def one(group, _):
                held = pl.ds(pl.multiple_of(group * LOW, LOW), LOW)
                left = left_col[held, :]
                parts = butterfly([stage[hi, held, :] for hi in range(count)])
                for hi, part in enumerate(parts):
                    part = (part * left).astype(jnp.bfloat16)
                    for begin in range(0, INNER, 128):
                        index, offset = divmod(hi * INNER + begin, piece)
                        chunk, dest = divmod(index, ring)
                        out = outs[chunk * ring + (dest - here) % ring]
                        out[held, offset : offset + 128] = part[:, begin : begin + 128]
                return 0

            lax.fori_loop(0, tile // LOW, one, 0, unroll=2)

        for here in range(ring):
            pl.when(mine == here)(lambda here=here: finish(here))

    pieces = chunks * ring
    operands = [place, weights, left_bits, right_bits]
    in_specs = [
        pl.BlockSpec(memory_space=pltpu.SMEM),
        pl.BlockSpec((tile, width), lambda r: (r + skip, 0)),
        pl.BlockSpec((1, tile), lambda r: (0, r + skip)),
        pl.BlockSpec((1, width), lambda r: (0, 0)),
    ]
    aliases = {}
    if before is not None:
        aliases = {len(operands) + k: ring + k for k in range(len(before))}
        operands += list(before)
        in_specs += [pl.BlockSpec(memory_space=pl.ANY)] * len(before)
    outs = pl.pallas_call(
        kernel,
        grid=(rows // tile,),
        in_specs=in_specs,
        out_specs=[pl.BlockSpec((tile, piece), lambda r: (r, 0))] * ring
        + [pl.BlockSpec((tile, piece), lambda r: (r + skip, 0))] * (pieces - ring),
        out_shape=[jax.ShapeDtypeStruct((rows, piece), jnp.bfloat16)] * ring
        + [jax.ShapeDtypeStruct((all_rows, piece), jnp.bfloat16)] * (pieces - ring),
        scratch_shapes=[
            pltpu.VMEM((INNER, INNER), jnp.bfloat16),
            pltpu.VMEM((count, tile, INNER), jnp.float32),
            pltpu.VMEM((tile, INNER), jnp.float32),
        ],
        input_output_aliases=aliases,
        name="column_transform",
    )(*operands)
    return outs[:ring], outs[ring:]


def row_mix(pieces, mixer, own_groups, before, splits):
    ring = len(pieces)
    width = pieces[0][0].shape[1]
    blocks = sum(splits)
    high = HB // LOW
    band = blocks * LOW
    root = 1.0 / math.sqrt(HB)
    flat = [p.reshape(p.shape[0] // HB, high, LOW, width) for piece in pieces for p in piece]

    def kernel(*refs):
        ins = refs[: len(flat)]
        m_ref, group_ref, before_ref = refs[len(flat) : len(flat) + 3]
        outs, peak_ref, stage = refs[len(flat) + 3 : -2], refs[-2], refs[-1]
        for hi in range(high):
            rhs = jnp.concatenate([r[:, hi].reshape(r.shape[0] * LOW, width) for r in ins], axis=0)
            stage[hi] = jnp.dot(m_ref[...], rhs, preferred_element_type=jnp.float32)

        peak = jnp.zeros((LOW, width), jnp.float32)
        for index, out in enumerate(outs):
            shift, split = divmod(index, len(splits))
            base = shift * band + sum(splits[:split]) * LOW

            def one(a, peak):
                start = pl.multiple_of(base + a * LOW, LOW)
                parts = butterfly([stage[hi, pl.ds(start, LOW), :] for hi in range(high)])
                for hi, part in enumerate(parts):
                    part = part * root
                    peak = jnp.maximum(peak, jnp.abs(part))
                    out[a, hi] = part.astype(jnp.bfloat16)
                return peak

            peak = lax.fori_loop(0, splits[split], one, peak)
        column_peak = jnp.max(peak, axis=0, keepdims=True)
        ids = lax.broadcasted_iota(jnp.int32, (GROUPS, width), 0)
        held = jnp.max(jnp.where(group_ref[...] == ids, column_peak, 0.0), axis=1, keepdims=True)
        peak_ref[...] = jnp.maximum(before_ref[...], held)

    result = pl.pallas_call(
        kernel,
        out_shape=[jax.ShapeDtypeStruct((n, high, LOW, width), jnp.bfloat16) for n in splits] * ring
        + [jax.ShapeDtypeStruct((GROUPS, 128), jnp.float32)],
        scratch_shapes=[pltpu.VMEM((high, ring * band, width), jnp.float32)],
        name="row_mix",
    )(*flat, mixer, own_groups, before)
    mixed = [y.reshape(y.shape[0] * HB, width) for y in result[:-1]]
    return [mixed[s * len(splits) : (s + 1) * len(splits)] for s in range(ring)], result[-1]


def quantize(part_index, pieces, scale_row, scale_octet, spread, numbers, before, first_row, rows, all_rows, tile):
    each = len(pieces)
    ring = len(pieces[0])
    piece = pieces[0][0].shape[1]
    skip = first_row // tile
    width = each * ring * piece
    lanes = width // OCTET
    parts_in_all = scale_row.shape[1] // width
    flat = [p for chunk in pieces for p in chunk]

    def kernel(num_ref, *refs):
        ins = refs[: each * ring]
        row_ref, oct_ref, spread_ref = refs[each * ring : each * ring + 3]
        scaled_ref, error_ref, sum_ref, stage = refs[-4:]
        mine, first, total = num_ref[0], num_ref[1], num_ref[2]
        step = pl.program_id(0)
        stage[...] = jnp.dot(
            jnp.concatenate([r[...] for r in ins], axis=1), spread_ref[...], preferred_element_type=jnp.float32
        )
        starts = []
        for index in range(each * ring):
            owner = lax.rem(mine - index % ring + ring, ring)
            starts.append(pl.multiple_of((index // ring * ring + owner) * piece, 128))
        share = 4.0 / (3.0 * total.astype(jnp.float32))

        def one(group, carry):
            held = pl.ds(pl.multiple_of(group * LOW, LOW), LOW)
            for index in range(each * ring):
                cols = pl.ds(starts[index], piece)
                scaled = ins[index][held, :].astype(jnp.float32) * row_ref[:, cols]
                scaled_ref[held, cols] = scaled.astype(jnp.bfloat16)
            near_sum = low_sum = squares = far_squares = largest = smallest = None
            for i in range(OCTET):
                value = stage[held, i * lanes : (i + 1) * lanes] * oct_ref[i : i + 1, :]
                near = jnp.floor(value + 0.5)
                low = jnp.floor(value)
                gap = jnp.abs(value - near)
                far = 0.5 - gap
                if i == 0:
                    near_sum, low_sum, squares, far_squares = near, low, gap * gap, far * far
                    largest = smallest = gap
                else:
                    near_sum, low_sum = near_sum + near, low_sum + low
                    squares, far_squares = squares + gap * gap, far_squares + far * far
                    largest, smallest = jnp.maximum(largest, gap), jnp.minimum(smallest, gap)
            near_half, low_half = near_sum * 0.5, low_sum * 0.5
            whole = jnp.where(near_half != jnp.floor(near_half), squares + (1.0 - 2.0 * largest), squares)
            shifted = jnp.where(low_half != jnp.floor(low_half), far_squares + 2.0 * smallest, far_squares)
            error = jnp.minimum(whole, shifted)
            error_ref[held, :] = error
            position = lax.broadcasted_iota(jnp.int32, (LOW, lanes), 0) + (first + first_row + step * tile + group * LOW)
            weight = (position.astype(jnp.float32) + 0.5) * share + (1.0 / 3.0)
            return carry + error * weight

        part = lax.fori_loop(0, tile // LOW, one, jnp.zeros((LOW, lanes), jnp.float32), unroll=2)

        @pl.when(step == 0)
        def _():
            sum_ref[...] = jnp.zeros_like(sum_ref)

        sum_ref[...] += part

    in_specs = [pl.BlockSpec(memory_space=pltpu.SMEM)]
    for p in flat:
        in_specs.append(pl.BlockSpec((tile, piece), lambda r, o=skip * (p.shape[0] == all_rows): (r + o, 0)))
    in_specs += [
        pl.BlockSpec((1, width), lambda r: (0, part_index)),
        pl.BlockSpec((OCTET, lanes), lambda r: (0, part_index)),
        pl.BlockSpec((width, width), lambda r: (0, 0)),
    ]
    operands = [numbers, *flat, scale_row, scale_octet, spread]
    aliases = {}
    if before is not None:
        aliases = {len(operands): 0, len(operands) + 1: 1}
        in_specs += [pl.BlockSpec(memory_space=pl.ANY)] * 2
        operands += list(before)
    return pl.pallas_call(
        kernel,
        grid=(rows // tile,),
        in_specs=in_specs,
        out_specs=[
            pl.BlockSpec((tile, width), lambda r: (r + skip, part_index)),
            pl.BlockSpec((tile, lanes), lambda r: (r + skip, part_index)),
            pl.BlockSpec((LOW, lanes), lambda r: (0, 0)),
        ],
        out_shape=[
            jax.ShapeDtypeStruct((all_rows, parts_in_all * width), jnp.bfloat16),
            jax.ShapeDtypeStruct((all_rows, parts_in_all * lanes), jnp.float32),
            jax.ShapeDtypeStruct((LOW, lanes), jnp.float32),
        ],
        scratch_shapes=[pltpu.VMEM((tile, width), jnp.float32)],
        input_output_aliases=aliases,
        name="quantize",
    )(*operands)


def mixer_table(mine, ring, blocks):
    side = ring * blocks * LOW
    row = lax.broadcasted_iota(jnp.int32, (side, side), 0)
    col = lax.broadcasted_iota(jnp.int32, (side, side), 1)
    band = blocks * LOW
    first = (((mine + row // band) % ring) * blocks + (row % band) // LOW).astype(jnp.float32)
    second = (((mine - col // band + ring) % ring) * blocks + (col % band) // LOW).astype(jnp.float32)
    order = ring * blocks
    table = math.sqrt(2.0 / order) * jnp.cos(math.pi * (2.0 * second + 1.0) * first / (2.0 * order))
    table = jnp.where(first == 0.0, table * math.sqrt(0.5), table)
    common = (row % LOW) & (col % LOW)
    common = common ^ (common >> 2)
    common = common ^ (common >> 1)
    return jnp.where((common & 1) == 0, table, -table).astype(jnp.bfloat16)


def spread_table(mine, ring, piece, width):
    row = lax.broadcasted_iota(jnp.int32, (width, width), 0)
    col = lax.broadcasted_iota(jnp.int32, (width, width), 1)
    index = row // piece
    natural = (index // ring * ring + (mine - index % ring + ring) % ring) * piece + row % piece
    target = (natural % OCTET) * (width // OCTET) + natural // OCTET
    return (target == col).astype(jnp.bfloat16)


def body(weights, left_bits, right_bits, groups):
    experts, local_rows, width = weights.shape
    assert experts == 1
    ring = lax.axis_size("row")
    mine = lax.axis_index("row").astype(jnp.int32)
    blocks_here = local_rows // HB
    chunks = chunk_count(width, ring)
    piece = width // (chunks * ring)
    unit = OCTET * 128
    each = unit // (ring * piece)
    place = mine.reshape(1)

    def send(x, shift):
        return lax.ppermute(x, "row", [(k, (k + shift) % ring) for k in range(ring)])

    splits = (blocks_here // 2, blocks_here - blocks_here // 2)
    halves = [n * HB for n in splits]
    step_rows = math.gcd(*halves)
    column_args = (weights[0], left_bits, right_bits, place, ring, chunks)
    early, whole = column_transform(*column_args, 0, halves[0], step_rows, None)
    late, whole = column_transform(*column_args, halves[0], halves[1], step_rows, whole)
    outgoing = [[[early[s], late[s]] for s in range(ring)]]
    outgoing += [[[whole[c * ring + s]] for s in range(ring)] for c in range(chunks - 1)]
    mixer = mixer_table(mine, ring, blocks_here)
    spread = spread_table(mine, ring, piece, unit)
    own_groups = [
        lax.dynamic_slice_in_dim(groups, (chunk * ring + mine) * piece, piece, 1) for chunk in range(chunks)
    ]
    received, returned = [], []
    for chunk in range(chunks):
        leaving = outgoing[chunk][1:]
        if chunk >= AHEAD:
            leaving, received[chunk - AHEAD] = lax.optimization_barrier((leaving, received[chunk - AHEAD]))
        arrived = [[] for _ in range(1, ring)]
        for part in range(len(leaving[0])):
            for s in range(1, ring):
                arrived[s - 1].append(send(leaving[s - 1][part], s))
        received.append(arrived)
    peak = jnp.zeros((GROUPS, 128), jnp.float32)
    for chunk in range(chunks):
        last = chunk == chunks - 1
        mixed, peak = row_mix(
            [outgoing[chunk][0]] + received[chunk],
            mixer,
            own_groups[chunk],
            peak,
            splits if last else (blocks_here,),
        )
        if last:
            peaks = [peak] + [send(peak, s) for s in range(1, ring)]
        back = []
        for part in range(len(mixed[0])):
            back.append([mixed[0][part]] + [send(mixed[s][part], s) for s in range(1, ring)])
        returned.append(back)

    group_peak = jnp.max(jnp.stack(peaks), axis=(0, 2))
    group_peak = jnp.maximum(group_peak, 1.0)
    in_group = groups == jnp.arange(GROUPS, dtype=jnp.int32)[:, None]
    scale_row = jnp.sum(jnp.where(in_group, (2.0 / group_peak)[:, None], 0.0), axis=0)
    scale_octet = scale_row.reshape(width // OCTET, OCTET).T

    numbers = jnp.stack([mine, mine * local_rows, jnp.int32(local_rows) * ring])
    before, total = None, 0.0
    fine = even_tile(step_rows, TILE2)
    for part_index in range(width // unit):
        held = returned[part_index * each : (part_index + 1) * each]
        ranges = [(0, local_rows)]
        if len(held[-1]) > 1:
            ranges = [(0, halves[0]), (halves[0], halves[1])]
        for part, (first_row, count) in enumerate(ranges):
            scaled, errors, share = quantize(
                part_index,
                [chunk[part % len(chunk)] for chunk in held],
                scale_row[None, :],
                scale_octet,
                spread,
                numbers,
                before,
                first_row,
                count,
                local_rows,
                fine,
            )
            before = (scaled, errors)
            total = total + share
    partial_error = jnp.sum(total) / (local_rows * ring * width // OCTET)
    expert_count = lax.axis_size("expert")
    copies = jnp.broadcast_to(partial_error, (expert_count * ring, 1))
    every_error = lax.all_to_all(copies, ("expert", "row"), 0, 0)
    every_error = jnp.sum(every_error.reshape(expert_count, ring), axis=1)
    expert_error = lax.dynamic_slice_in_dim(every_error, lax.axis_index("expert"), 1)
    total_error = jnp.sum(every_error) / expert_count
    return (scaled[None], errors[None], (group_peak / 2.0)[None], expert_error, total_error)


def chunk_count(width, ring):
    return min(CHUNKS, width // (128 * ring))


def solution(mesh):
    placed = (P("expert", "row", None), P("expert", "row"), P("expert", None), P("expert", None))
    return jax.shard_map(
        body,
        mesh=mesh,
        in_specs=placed,
        out_specs=(
            P("expert", "row", None),
            P("expert", "row", None),
            P("expert", None),
            P("expert"),
            P(),
        ),
        check_vma=False,
    )
```

```python
import math

import jax
import jax.numpy as jnp
from jax import lax
from jax.experimental import pallas as pl
from jax.experimental.pallas import tpu as pltpu
from jax.sharding import PartitionSpec as P

HB = 128
GROUPS = 16
INNER = 256
LOW = 16
CHUNKS = 4
AHEAD = 2
OCTET = 8
TILE2 = 448


def butterfly(parts):
    parts = list(parts)
    step = 1
    while step < len(parts):
        for base in range(len(parts)):
            if not base & step:
                low, high = parts[base], parts[base | step]
                parts[base], parts[base | step] = low + high, low - high
        step *= 2
    return parts


def even_tile(rows, most):
    return max(t for t in range(HB, most + 1, HB // 2) if rows % t == 0)


def column_transform(weights, left_bits, right_bits, place, ring, chunks, first, rows, tile, before):
    all_rows, width = weights.shape
    skip = first // tile
    count = width // INNER
    piece = width // (chunks * ring)
    root = 1.0 / math.sqrt(width)

    def kernel(place_ref, w_ref, left_ref, right_ref, *rest):
        rest = rest[0 if before is None else len(before) :]
        outs = rest[: chunks * ring]
        table, stage, left_col = rest[chunks * ring :]
        mine = place_ref[0]

        @pl.when(pl.program_id(0) == 0)
        def _():
            common = lax.broadcasted_iota(jnp.int32, (INNER, INNER), 0) & lax.broadcasted_iota(
                jnp.int32, (INNER, INNER), 1
            )
            for bits in (4, 2, 1):
                common = common ^ (common >> bits)
            table[...] = (1 - 2 * (common & 1)).astype(jnp.float32).astype(jnp.bfloat16)

        eye = lax.broadcasted_iota(jnp.int32, (HB, HB), 0) == lax.broadcasted_iota(jnp.int32, (HB, HB), 1)
        for part in range(tile // HB):
            cols = slice(part * HB, (part + 1) * HB)
            signs = (2 * left_ref[:, cols] - 1).astype(jnp.float32) * root
            column = jnp.sum(jnp.where(eye, signs, 0.0), axis=1, keepdims=True)
            left_col[cols, :] = jnp.broadcast_to(column, (HB, INNER))
        right = (2 * right_ref[...] - 1).astype(jnp.float32).astype(jnp.bfloat16)
        signed = [
            w_ref[:, hi * INNER : (hi + 1) * INNER] * right[:, hi * INNER : (hi + 1) * INNER]
            for hi in range(count)
        ]
        turned = jnp.dot(jnp.concatenate(signed, axis=0), table[...], preferred_element_type=jnp.float32)
        stage[...] = turned.reshape(count, tile, INNER)

        def finish(here):
            def one(group, _):
                held = pl.ds(pl.multiple_of(group * LOW, LOW), LOW)
                left = left_col[held, :]
                parts = butterfly([stage[hi, held, :] for hi in range(count)])
                for hi, part in enumerate(parts):
                    part = (part * left).astype(jnp.bfloat16)
                    for begin in range(0, INNER, 128):
                        index, offset = divmod(hi * INNER + begin, piece)
                        chunk, dest = divmod(index, ring)
                        out = outs[chunk * ring + (dest - here) % ring]
                        out[held, offset : offset + 128] = part[:, begin : begin + 128]
                return 0

            lax.fori_loop(0, tile // LOW, one, 0, unroll=2)

        for here in range(ring):
            pl.when(mine == here)(lambda here=here: finish(here))

    pieces = chunks * ring
    operands = [place, weights, left_bits, right_bits]
    in_specs = [
        pl.BlockSpec(memory_space=pltpu.SMEM),
        pl.BlockSpec((tile, width), lambda r: (r + skip, 0)),
        pl.BlockSpec((1, tile), lambda r: (0, r + skip)),
        pl.BlockSpec((1, width), lambda r: (0, 0)),
    ]
    aliases = {}
    if before is not None:
        aliases = {len(operands) + k: ring + k for k in range(len(before))}
        operands += list(before)
        in_specs += [pl.BlockSpec(memory_space=pl.ANY)] * len(before)
    outs = pl.pallas_call(
        kernel,
        grid=(rows // tile,),
        in_specs=in_specs,
        out_specs=[pl.BlockSpec((tile, piece), lambda r: (r, 0))] * ring
        + [pl.BlockSpec((tile, piece), lambda r: (r + skip, 0))] * (pieces - ring),
        out_shape=[jax.ShapeDtypeStruct((rows, piece), jnp.bfloat16)] * ring
        + [jax.ShapeDtypeStruct((all_rows, piece), jnp.bfloat16)] * (pieces - ring),
        scratch_shapes=[
            pltpu.VMEM((INNER, INNER), jnp.bfloat16),
            pltpu.VMEM((count, tile, INNER), jnp.float32),
            pltpu.VMEM((tile, INNER), jnp.float32),
        ],
        input_output_aliases=aliases,
        name="column_transform",
    )(*operands)
    return outs[:ring], outs[ring:]


def row_mix(pieces, mixer, own_groups, before, splits):
    ring = len(pieces)
    width = pieces[0][0].shape[1]
    blocks = sum(splits)
    high = HB // LOW
    band = blocks * LOW
    root = 1.0 / math.sqrt(HB)
    flat = [p.reshape(p.shape[0] // HB, high, LOW, width) for piece in pieces for p in piece]

    def kernel(*refs):
        ins = refs[: len(flat)]
        m_ref, group_ref, before_ref = refs[len(flat) : len(flat) + 3]
        outs, peak_ref, stage = refs[len(flat) + 3 : -2], refs[-2], refs[-1]
        for hi in range(high):
            rhs = jnp.concatenate([r[:, hi].reshape(r.shape[0] * LOW, width) for r in ins], axis=0)
            stage[hi] = jnp.dot(m_ref[...], rhs, preferred_element_type=jnp.float32)

        peak = jnp.zeros((LOW, width), jnp.float32)
        for index, out in enumerate(outs):
            shift, split = divmod(index, len(splits))
            base = shift * band + sum(splits[:split]) * LOW

            def one(a, peak):
                start = pl.multiple_of(base + a * LOW, LOW)
                parts = butterfly([stage[hi, pl.ds(start, LOW), :] for hi in range(high)])
                for hi, part in enumerate(parts):
                    part = part * root
                    peak = jnp.maximum(peak, jnp.abs(part))
                    out[a, hi] = part.astype(jnp.bfloat16)
                return peak

            peak = lax.fori_loop(0, splits[split], one, peak)
        column_peak = jnp.max(peak, axis=0, keepdims=True)
        ids = lax.broadcasted_iota(jnp.int32, (GROUPS, width), 0)
        held = jnp.max(jnp.where(group_ref[...] == ids, column_peak, 0.0), axis=1, keepdims=True)
        peak_ref[...] = jnp.maximum(before_ref[...], held)

    result = pl.pallas_call(
        kernel,
        out_shape=[jax.ShapeDtypeStruct((n, high, LOW, width), jnp.bfloat16) for n in splits] * ring
        + [jax.ShapeDtypeStruct((GROUPS, 128), jnp.float32)],
        scratch_shapes=[pltpu.VMEM((high, ring * band, width), jnp.float32)],
        name="row_mix",
    )(*flat, mixer, own_groups, before)
    mixed = [y.reshape(y.shape[0] * HB, width) for y in result[:-1]]
    return [mixed[s * len(splits) : (s + 1) * len(splits)] for s in range(ring)], result[-1]


def octet_error(values):
    near_sum = low_sum = squares = far_squares = largest = smallest = None
    for value in values:
        near = jnp.floor(value + 0.5)
        low = jnp.floor(value)
        gap = jnp.abs(value - near)
        far = 0.5 - gap
        if near_sum is None:
            near_sum, low_sum, squares, far_squares = near, low, gap * gap, far * far
            largest = smallest = gap
        else:
            near_sum, low_sum = near_sum + near, low_sum + low
            squares, far_squares = squares + gap * gap, far_squares + far * far
            largest, smallest = jnp.maximum(largest, gap), jnp.minimum(smallest, gap)
    near_half, low_half = near_sum * 0.5, low_sum * 0.5
    whole = jnp.where(near_half != jnp.floor(near_half), squares + (1.0 - 2.0 * largest), squares)
    shifted = jnp.where(low_half != jnp.floor(low_half), far_squares + 2.0 * smallest, far_squares)
    return jnp.minimum(whole, shifted)


def quantize(chunk, pieces, scale_row, scale_octet, spread, place, before, halves_error, first_row, rows, tile):
    ring = len(pieces)
    piece = pieces[0].shape[1]
    all_rows, all_width = before[2]
    width = ring * piece
    fold = OCTET * 128 // width
    lanes = width // OCTET
    skip = first_row // tile
    band = tile // fold
    closing = chunk % fold == fold - 1

    def kernel(place_ref, *refs):
        ins = refs[:ring]
        row_ref, oct_ref, spread_ref = refs[ring : ring + 3]
        half_ref = refs[ring + 3] if halves_error is not None else None
        scaled_ref, error_ref, stage = refs[-3:]
        mine = place_ref[0]
        bands = [r[f * band : (f + 1) * band, :] for f in range(fold) for r in ins]
        stage[...] = jnp.dot(
            jnp.concatenate(bands, axis=1), spread_ref[...], preferred_element_type=jnp.float32
        )
        starts = [pl.multiple_of(lax.rem(mine - s + ring, ring) * piece, 128) for s in range(ring)]

        def one(group, _):
            start = pl.multiple_of(group * LOW, LOW)
            for f in range(fold):
                held = pl.ds(f * band + start, LOW)
                for s in range(ring):
                    cols = pl.ds(starts[s], piece)
                    scaled = ins[s][held, :].astype(jnp.float32) * row_ref[:, cols]
                    scaled_ref[held, cols] = scaled.astype(jnp.bfloat16)
            held = pl.ds(start, LOW)
            error = octet_error(stage[held, i * 128 : (i + 1) * 128] * oct_ref[i : i + 1, :] for i in range(OCTET))
            if fold == 1 or not closing:
                error_ref[held, :] = error
            else:
                other = half_ref[held, :]
                left = lax.broadcasted_iota(jnp.int32, (LOW, 128), 1) < lanes
                error_ref[held, :] = jnp.where(left, other, pltpu.roll(error, lanes, 1))
                error_ref[pl.ds(band + start, LOW), :] = jnp.where(left, pltpu.roll(other, lanes, 1), error)
            return 0

        lax.fori_loop(0, band // LOW, one, 0, unroll=2)

    in_specs = [pl.BlockSpec(memory_space=pltpu.SMEM)]
    for p in pieces:
        in_specs.append(pl.BlockSpec((tile, piece), lambda r, o=skip * (p.shape[0] == all_rows): (r + o, 0)))
    in_specs += [
        pl.BlockSpec((1, width), lambda r: (0, chunk)),
        pl.BlockSpec((OCTET, 128), lambda r: (chunk, 0)),
        pl.BlockSpec((OCTET * 128, OCTET * 128), lambda r: (0, 0)),
    ]
    operands = [place, *pieces, scale_row, scale_octet, spread]
    if halves_error is not None:
        in_specs.append(pl.BlockSpec((band, 128), lambda r: (r + skip, 0)))
        operands.append(halves_error)
    aliases = {}
    if before[0] is not None:
        aliases[len(operands)] = 0
        in_specs.append(pl.BlockSpec(memory_space=pl.ANY))
        operands.append(before[0])
    if closing:
        error_spec = pl.BlockSpec((tile, 128), lambda r: (r + skip, chunk // fold))
        error_shape = (all_rows, all_width // OCTET)
        if before[1] is not None:
            aliases[len(operands)] = 1
            in_specs.append(pl.BlockSpec(memory_space=pl.ANY))
            operands.append(before[1])
    else:
        error_spec = pl.BlockSpec((band, 128), lambda r: (r + skip, 0))
        error_shape = (all_rows // fold, 128)
    scaled, errors = pl.pallas_call(
        kernel,
        grid=(rows // tile,),
        in_specs=in_specs,
        out_specs=[pl.BlockSpec((tile, width), lambda r: (r + skip, chunk)), error_spec],
        out_shape=[
            jax.ShapeDtypeStruct((all_rows, all_width), jnp.bfloat16),
            jax.ShapeDtypeStruct(error_shape, jnp.float32),
        ],
        scratch_shapes=[pltpu.VMEM((band, OCTET * 128), jnp.float32)],
        input_output_aliases=aliases,
        name="quantize",
    )(*operands)
    if closing:
        return (scaled, errors, before[2]), None
    return (scaled, before[1], before[2]), errors


def lattice_sum(pieces, scale_own, spread_own, place, first_row, rows, tile, all_rows):
    ring = len(pieces)
    piece = pieces[0][0].shape[1]
    own = len(pieces[0]) * piece
    fold = OCTET * 128 // own
    skip = first_row // tile
    share = 4.0 / (3.0 * all_rows * ring)
    flat = [p for owner in pieces for p in owner]

    def kernel(place_ref, *refs):
        ins, oct_ref, spread_ref, sum_ref, stage = refs[: len(flat)], *refs[len(flat) :]
        mine = place_ref[0]
        step = pl.program_id(0)

        @pl.when(step == 0)
        def _():
            sum_ref[...] = jnp.zeros_like(sum_ref)

        lane = lax.broadcasted_iota(jnp.int32, (LOW, 128), 1)
        inside = lax.broadcasted_iota(jnp.int32, (LOW, 128), 0)
        each = len(flat) // ring * fold
        for group in range(ring // fold):
            stage[...] = jnp.dot(
                jnp.concatenate([r[...] for r in ins[group * each : (group + 1) * each]], axis=1),
                spread_ref[...],
                preferred_element_type=jnp.float32,
            )
            owner = mine + (group * fold + lane // (128 // fold))
            owner = jnp.where(owner >= ring, owner - ring, owner)
            position = owner * all_rows + inside + (first_row + step * tile)

            def one(index, carry):
                held = pl.ds(pl.multiple_of(index * LOW, LOW), LOW)
                error = octet_error(
                    stage[held, i * 128 : (i + 1) * 128] * oct_ref[i : i + 1, :] for i in range(OCTET)
                )
                weight = ((position + index * LOW).astype(jnp.float32) + 0.5) * share + (1.0 / 3.0)
                return carry + error * weight

            sum_ref[...] += lax.fori_loop(0, tile // LOW, one, jnp.zeros((LOW, 128), jnp.float32), unroll=2)

    in_specs = [pl.BlockSpec(memory_space=pltpu.SMEM)]
    for p in flat:
        in_specs.append(pl.BlockSpec((tile, piece), lambda r, o=skip * (p.shape[0] == all_rows): (r + o, 0)))
    in_specs += [
        pl.BlockSpec((OCTET, 128), lambda r: (0, 0)),
        pl.BlockSpec((OCTET * 128, OCTET * 128), lambda r: (0, 0)),
    ]
    return pl.pallas_call(
        kernel,
        grid=(rows // tile,),
        in_specs=in_specs,
        out_specs=pl.BlockSpec((LOW, 128), lambda r: (0, 0)),
        out_shape=jax.ShapeDtypeStruct((LOW, 128), jnp.float32),
        scratch_shapes=[pltpu.VMEM((tile, OCTET * 128), jnp.float32)],
        name="lattice_sum",
    )(place, *flat, scale_own, spread_own)


def mixer_table(mine, ring, blocks):
    side = ring * blocks * LOW
    row = lax.broadcasted_iota(jnp.int32, (side, side), 0)
    col = lax.broadcasted_iota(jnp.int32, (side, side), 1)
    band = blocks * LOW
    first = (((mine + row // band) % ring) * blocks + (row % band) // LOW).astype(jnp.float32)
    second = (((mine - col // band + ring) % ring) * blocks + (col % band) // LOW).astype(jnp.float32)
    order = ring * blocks
    table = math.sqrt(2.0 / order) * jnp.cos(math.pi * (2.0 * second + 1.0) * first / (2.0 * order))
    table = jnp.where(first == 0.0, table * math.sqrt(0.5), table)
    common = (row % LOW) & (col % LOW)
    common = common ^ (common >> 2)
    common = common ^ (common >> 1)
    return jnp.where((common & 1) == 0, table, -table).astype(jnp.bfloat16)


def spread_table(natural, fold):
    side = OCTET * 128
    width = side // fold
    row = lax.broadcasted_iota(jnp.int32, (side, side), 0)
    col = lax.broadcasted_iota(jnp.int32, (side, side), 1)
    column = natural(row % width)
    target = (column % OCTET) * 128 + (row // width) * (width // OCTET) + column // OCTET
    return (target == col).astype(jnp.bfloat16)


def octet_rows(scales):
    turned = jnp.swapaxes(scales.reshape(scales.shape[:-1] + (-1, OCTET)), -1, -2)
    return jnp.concatenate([turned] * (128 // turned.shape[-1]), axis=-1)


def body(weights, left_bits, right_bits, groups):
    experts, local_rows, width = weights.shape
    assert experts == 1
    ring = lax.axis_size("row")
    mine = lax.axis_index("row").astype(jnp.int32)
    blocks_here = local_rows // HB
    chunks = chunk_count(width, ring)
    piece = width // (chunks * ring)
    place = mine.reshape(1)

    def send(x, shift):
        return lax.ppermute(x, "row", [(k, (k + shift) % ring) for k in range(ring)])

    column_args = (weights[0], left_bits, right_bits, place, ring, chunks)
    start_rows = max(blocks_here * 2 // 7, 1) * HB
    early, whole = column_transform(*column_args, 0, start_rows, start_rows, None)
    left_rows = local_rows - start_rows
    late, whole = column_transform(
        *column_args, start_rows, left_rows, math.gcd(start_rows, left_rows), whole
    )
    splits = (blocks_here // 2, blocks_here - blocks_here // 2)
    halves = [n * HB for n in splits]
    step_rows = math.gcd(*halves)
    outgoing = [[[early[s], late[s]] for s in range(ring)]]
    outgoing += [[[whole[c * ring + s]] for s in range(ring)] for c in range(chunks - 1)]
    mixer = mixer_table(mine, ring, blocks_here)
    band_columns = ring * piece
    spread = spread_table(
        lambda at: (mine - at // piece + ring) % ring * piece + at % piece, OCTET * 128 // band_columns
    )
    spread_own = spread_table(lambda at: at, OCTET * 128 // (chunks * piece))
    own_groups = [
        lax.dynamic_slice_in_dim(groups, (chunk * ring + mine) * piece, piece, 1) for chunk in range(chunks)
    ]
    received, returned, kept = [], [], []
    for chunk in range(chunks):
        leaving = outgoing[chunk][1:]
        if chunk >= AHEAD:
            leaving, received[chunk - AHEAD] = lax.optimization_barrier((leaving, received[chunk - AHEAD]))
        arrived = [[] for _ in range(1, ring)]
        for part in range(len(leaving[0])):
            for s in range(1, ring):
                arrived[s - 1].append(send(leaving[s - 1][part], s))
        received.append(arrived)
    peak = jnp.zeros((GROUPS, 128), jnp.float32)
    for chunk in range(chunks):
        last = chunk == chunks - 1
        mixed, peak = row_mix(
            [outgoing[chunk][0]] + received[chunk],
            mixer,
            own_groups[chunk],
            peak,
            splits if last else (blocks_here,),
        )
        if last:
            peaks = [peak] + [send(peak, s) for s in range(1, ring)]
        kept.append(mixed)
        back = []
        for part in range(len(mixed[0])):
            back.append([mixed[0][part]] + [send(mixed[s][part], s) for s in range(1, ring)])
        returned.append(back)

    group_peak = jnp.max(jnp.stack(peaks), axis=(0, 2))
    group_peak = jnp.maximum(group_peak, 1.0)
    in_group = groups == jnp.arange(GROUPS, dtype=jnp.int32)[:, None]
    scale_row = jnp.sum(jnp.where(in_group, (2.0 / group_peak)[:, None], 0.0), axis=0)
    scale_octet = octet_rows(scale_row.reshape(chunks, band_columns)).reshape(chunks * OCTET, 128)
    own_scale = lax.dynamic_slice_in_dim(scale_row.reshape(chunks, ring, piece), mine, 1, 1)
    scale_own = octet_rows(own_scale.reshape(chunks * piece))

    fine = even_tile(step_rows, TILE2)
    ranges = [(0, halves[0]), (halves[0], halves[1])]
    shares = []
    for part, (first_row, count) in enumerate(ranges):
        own_pieces = [[k[s][part % len(k[s])] for k in kept] for s in range(ring)]
        shares.append(
            lattice_sum(own_pieces, scale_own, spread_own, place, first_row, count, fine, local_rows)
        )
    partial_error = jnp.sum(sum(shares)) / (local_rows * ring * width // OCTET)
    expert_count = lax.axis_size("expert")
    copies = jnp.broadcast_to(partial_error, (expert_count * ring, 1))
    every_error = lax.all_to_all(copies, ("expert", "row"), 0, 0)
    every_error = jnp.sum(every_error.reshape(expert_count, ring), axis=1)
    expert_error = lax.dynamic_slice_in_dim(every_error, lax.axis_index("expert"), 1)
    total_error = jnp.sum(every_error) / expert_count

    before, half_error = (None, None, (local_rows, width)), None
    for chunk in range(chunks):
        back = returned[chunk]
        spans = [(0, local_rows)] if len(back) == 1 else ranges
        given = half_error
        for part, (first_row, count) in enumerate(spans):
            before, half_error = quantize(
                chunk,
                back[part],
                scale_row[None, :],
                scale_octet,
                spread,
                place,
                before,
                given,
                first_row,
                count,
                fine,
            )
    scaled, errors, _ = before
    return (scaled[None], errors[None], (group_peak / 2.0)[None], expert_error, total_error)


def chunk_count(width, ring):
    return min(CHUNKS, width // (128 * ring))


def solution(mesh):
    placed = (P("expert", "row", None), P("expert", "row"), P("expert", None), P("expert", None))
    return jax.shard_map(
        body,
        mesh=mesh,
        in_specs=placed,
        out_specs=(
            P("expert", "row", None),
            P("expert", "row", None),
            P("expert", None),
            P("expert"),
            P(),
        ),
        check_vma=False,
    )
```

```python
import math

import jax
import jax.numpy as jnp
from jax import lax
from jax.experimental import pallas as pl
from jax.experimental.pallas import tpu as pltpu
from jax.sharding import PartitionSpec as P

HB = 128
GROUPS = 16
INNER = 256
LOW = 16
CHUNKS = 4
AHEAD = 2
OCTET = 8
TILE2 = 448


def butterfly(parts):
    parts = list(parts)
    step = 1
    while step < len(parts):
        for base in range(len(parts)):
            if not base & step:
                low, high = parts[base], parts[base | step]
                parts[base], parts[base | step] = low + high, low - high
        step *= 2
    return parts


def even_tile(rows, most):
    return max(t for t in range(HB, most + 1, HB // 2) if rows % t == 0)


def column_transform(weights, left_bits, right_bits, place, ring, chunks, first, rows, tile, before):
    all_rows, width = weights.shape
    skip = first // tile
    count = width // INNER
    piece = width // (chunks * ring)
    root = 1.0 / math.sqrt(width)

    def kernel(place_ref, w_ref, left_ref, right_ref, *rest):
        rest = rest[0 if before is None else len(before) :]
        outs = rest[: chunks * ring]
        table, stage, left_col = rest[chunks * ring :]
        mine = place_ref[0]

        @pl.when(pl.program_id(0) == 0)
        def _():
            common = lax.broadcasted_iota(jnp.int32, (INNER, INNER), 0) & lax.broadcasted_iota(
                jnp.int32, (INNER, INNER), 1
            )
            for bits in (4, 2, 1):
                common = common ^ (common >> bits)
            table[...] = (1 - 2 * (common & 1)).astype(jnp.float32).astype(jnp.bfloat16)

        eye = lax.broadcasted_iota(jnp.int32, (HB, HB), 0) == lax.broadcasted_iota(jnp.int32, (HB, HB), 1)
        for part in range(tile // HB):
            cols = slice(part * HB, (part + 1) * HB)
            signs = (2 * left_ref[:, cols] - 1).astype(jnp.float32) * root
            column = jnp.sum(jnp.where(eye, signs, 0.0), axis=1, keepdims=True)
            left_col[cols, :] = jnp.broadcast_to(column, (HB, INNER))
        right = (2 * right_ref[...] - 1).astype(jnp.float32).astype(jnp.bfloat16)
        signed = [
            w_ref[:, hi * INNER : (hi + 1) * INNER] * right[:, hi * INNER : (hi + 1) * INNER]
            for hi in range(count)
        ]
        turned = jnp.dot(jnp.concatenate(signed, axis=0), table[...], preferred_element_type=jnp.float32)
        stage[...] = turned.reshape(count, tile, INNER)

        def finish(here):
            def one(group, _):
                held = pl.ds(pl.multiple_of(group * LOW, LOW), LOW)
                left = left_col[held, :]
                parts = butterfly([stage[hi, held, :] for hi in range(count)])
                for hi, part in enumerate(parts):
                    part = (part * left).astype(jnp.bfloat16)
                    for begin in range(0, INNER, 128):
                        index, offset = divmod(hi * INNER + begin, piece)
                        chunk, dest = divmod(index, ring)
                        out = outs[chunk * ring + (dest - here) % ring]
                        out[held, offset : offset + 128] = part[:, begin : begin + 128]
                return 0

            lax.fori_loop(0, tile // LOW, one, 0, unroll=2)

        for here in range(ring):
            pl.when(mine == here)(lambda here=here: finish(here))

    pieces = chunks * ring
    operands = [place, weights, left_bits, right_bits]
    in_specs = [
        pl.BlockSpec(memory_space=pltpu.SMEM),
        pl.BlockSpec((tile, width), lambda r: (r + skip, 0)),
        pl.BlockSpec((1, tile), lambda r: (0, r + skip)),
        pl.BlockSpec((1, width), lambda r: (0, 0)),
    ]
    aliases = {}
    if before is not None:
        aliases = {len(operands) + k: ring + k for k in range(len(before))}
        operands += list(before)
        in_specs += [pl.BlockSpec(memory_space=pl.ANY)] * len(before)
    outs = pl.pallas_call(
        kernel,
        grid=(rows // tile,),
        in_specs=in_specs,
        out_specs=[pl.BlockSpec((tile, piece), lambda r: (r, 0))] * ring
        + [pl.BlockSpec((tile, piece), lambda r: (r + skip, 0))] * (pieces - ring),
        out_shape=[jax.ShapeDtypeStruct((rows, piece), jnp.bfloat16)] * ring
        + [jax.ShapeDtypeStruct((all_rows, piece), jnp.bfloat16)] * (pieces - ring),
        scratch_shapes=[
            pltpu.VMEM((INNER, INNER), jnp.bfloat16),
            pltpu.VMEM((count, tile, INNER), jnp.float32),
            pltpu.VMEM((tile, INNER), jnp.float32),
        ],
        input_output_aliases=aliases,
        name="column_transform",
    )(*operands)
    return outs[:ring], outs[ring:]


def row_mix(pieces, mixer, own_groups, before, splits):
    ring = len(pieces)
    width = pieces[0][0].shape[1]
    blocks = sum(splits)
    high = HB // LOW
    band = blocks * LOW
    root = 1.0 / math.sqrt(HB)
    flat = [p.reshape(p.shape[0] // HB, high, LOW, width) for piece in pieces for p in piece]

    def kernel(*refs):
        ins = refs[: len(flat)]
        m_ref, group_ref, before_ref = refs[len(flat) : len(flat) + 3]
        outs, peak_ref, stage = refs[len(flat) + 3 : -2], refs[-2], refs[-1]
        for hi in range(high):
            rhs = jnp.concatenate([r[:, hi].reshape(r.shape[0] * LOW, width) for r in ins], axis=0)
            stage[hi] = jnp.dot(m_ref[...], rhs, preferred_element_type=jnp.float32)

        peak = jnp.zeros((LOW, width), jnp.float32)
        for index, out in enumerate(outs):
            shift, split = divmod(index, len(splits))
            base = shift * band + sum(splits[:split]) * LOW

            def one(a, peak):
                start = pl.multiple_of(base + a * LOW, LOW)
                parts = butterfly([stage[hi, pl.ds(start, LOW), :] for hi in range(high)])
                for hi, part in enumerate(parts):
                    part = part * root
                    peak = jnp.maximum(peak, jnp.abs(part))
                    out[a, hi] = part.astype(jnp.bfloat16)
                return peak

            peak = lax.fori_loop(0, splits[split], one, peak)
        column_peak = jnp.max(peak, axis=0, keepdims=True)
        ids = lax.broadcasted_iota(jnp.int32, (GROUPS, width), 0)
        held = jnp.max(jnp.where(group_ref[...] == ids, column_peak, 0.0), axis=1, keepdims=True)
        peak_ref[...] = jnp.maximum(before_ref[...], held)

    result = pl.pallas_call(
        kernel,
        out_shape=[jax.ShapeDtypeStruct((n, high, LOW, width), jnp.bfloat16) for n in splits] * ring
        + [jax.ShapeDtypeStruct((GROUPS, 128), jnp.float32)],
        scratch_shapes=[pltpu.VMEM((high, ring * band, width), jnp.float32)],
        name="row_mix",
    )(*flat, mixer, own_groups, before)
    mixed = [y.reshape(y.shape[0] * HB, width) for y in result[:-1]]
    return [mixed[s * len(splits) : (s + 1) * len(splits)] for s in range(ring)], result[-1]


def octet_error(values):
    near_sum = low_sum = squares = far_squares = largest = smallest = None
    for value in values:
        near = jnp.floor(value + 0.5)
        low = jnp.floor(value)
        gap = jnp.abs(value - near)
        far = 0.5 - gap
        if near_sum is None:
            near_sum, low_sum, squares, far_squares = near, low, gap * gap, far * far
            largest = smallest = gap
        else:
            near_sum, low_sum = near_sum + near, low_sum + low
            squares, far_squares = squares + gap * gap, far_squares + far * far
            largest, smallest = jnp.maximum(largest, gap), jnp.minimum(smallest, gap)
    near_half, low_half = near_sum * 0.5, low_sum * 0.5
    whole = jnp.where(near_half != jnp.floor(near_half), squares + (1.0 - 2.0 * largest), squares)
    shifted = jnp.where(low_half != jnp.floor(low_half), far_squares + 2.0 * smallest, far_squares)
    return jnp.minimum(whole, shifted)


def quantize(chunk, pieces, scale_row, scale_octet, spread, place, before, halves_error, first_row, rows, tile):
    ring = len(pieces)
    piece = pieces[0].shape[1]
    all_rows, all_width = before[2]
    width = ring * piece
    fold = OCTET * 128 // width
    lanes = width // OCTET
    skip = first_row // tile
    band = tile // fold
    closing = chunk % fold == fold - 1

    def kernel(place_ref, *refs):
        ins = refs[:ring]
        row_ref, oct_ref, spread_ref = refs[ring : ring + 3]
        half_ref = refs[ring + 3] if halves_error is not None else None
        scaled_ref, error_ref, stage = refs[-3:]
        mine = place_ref[0]
        bands = [r[f * band : (f + 1) * band, :] for f in range(fold) for r in ins]
        stage[...] = jnp.dot(
            jnp.concatenate(bands, axis=1), spread_ref[...], preferred_element_type=jnp.float32
        )
        starts = [pl.multiple_of(lax.rem(mine - s + ring, ring) * piece, 128) for s in range(ring)]

        def one(group, _):
            start = pl.multiple_of(group * LOW, LOW)
            for f in range(fold):
                held = pl.ds(f * band + start, LOW)
                for s in range(ring):
                    cols = pl.ds(starts[s], piece)
                    scaled = ins[s][held, :].astype(jnp.float32) * row_ref[:, cols]
                    scaled_ref[held, cols] = scaled.astype(jnp.bfloat16)
            held = pl.ds(start, LOW)
            error = octet_error(stage[held, i * 128 : (i + 1) * 128] * oct_ref[i : i + 1, :] for i in range(OCTET))
            if fold == 1 or not closing:
                error_ref[held, :] = error
            else:
                other = half_ref[held, :]
                left = lax.broadcasted_iota(jnp.int32, (LOW, 128), 1) < lanes
                error_ref[held, :] = jnp.where(left, other, pltpu.roll(error, lanes, 1))
                error_ref[pl.ds(band + start, LOW), :] = jnp.where(left, pltpu.roll(other, lanes, 1), error)
            return 0

        lax.fori_loop(0, band // LOW, one, 0, unroll=True)

    in_specs = [pl.BlockSpec(memory_space=pltpu.SMEM)]
    for p in pieces:
        in_specs.append(pl.BlockSpec((tile, piece), lambda r, o=skip * (p.shape[0] == all_rows): (r + o, 0)))
    in_specs += [
        pl.BlockSpec((1, width), lambda r: (0, chunk)),
        pl.BlockSpec((OCTET, 128), lambda r: (chunk, 0)),
        pl.BlockSpec((OCTET * 128, OCTET * 128), lambda r: (0, 0)),
    ]
    operands = [place, *pieces, scale_row, scale_octet, spread]
    if halves_error is not None:
        in_specs.append(pl.BlockSpec((band, 128), lambda r: (r + skip, 0)))
        operands.append(halves_error)
    aliases = {}
    if before[0] is not None:
        aliases[len(operands)] = 0
        in_specs.append(pl.BlockSpec(memory_space=pl.ANY))
        operands.append(before[0])
    if closing:
        error_spec = pl.BlockSpec((tile, 128), lambda r: (r + skip, chunk // fold))
        error_shape = (all_rows, all_width // OCTET)
        if before[1] is not None:
            aliases[len(operands)] = 1
            in_specs.append(pl.BlockSpec(memory_space=pl.ANY))
            operands.append(before[1])
    else:
        error_spec = pl.BlockSpec((band, 128), lambda r: (r + skip, 0))
        error_shape = (all_rows // fold, 128)
    scaled, errors = pl.pallas_call(
        kernel,
        grid=(rows // tile,),
        in_specs=in_specs,
        out_specs=[pl.BlockSpec((tile, width), lambda r: (r + skip, chunk)), error_spec],
        out_shape=[
            jax.ShapeDtypeStruct((all_rows, all_width), jnp.bfloat16),
            jax.ShapeDtypeStruct(error_shape, jnp.float32),
        ],
        scratch_shapes=[pltpu.VMEM((band, OCTET * 128), jnp.float32)],
        input_output_aliases=aliases,
        name="quantize",
    )(*operands)
    if closing:
        return (scaled, errors, before[2]), None
    return (scaled, before[1], before[2]), errors


def lattice_sum(pieces, scale_own, spread_own, place, first_row, rows, tile, all_rows):
    ring = len(pieces)
    piece = pieces[0][0].shape[1]
    own = len(pieces[0]) * piece
    fold = OCTET * 128 // own
    skip = first_row // tile
    share = 4.0 / (3.0 * all_rows * ring)
    flat = [p for owner in pieces for p in owner]

    def kernel(place_ref, *refs):
        ins, oct_ref, spread_ref, sum_ref, stage = refs[: len(flat)], *refs[len(flat) :]
        mine = place_ref[0]
        step = pl.program_id(0)

        @pl.when(step == 0)
        def _():
            sum_ref[...] = jnp.zeros_like(sum_ref)

        lane = lax.broadcasted_iota(jnp.int32, (LOW, 128), 1)
        inside = lax.broadcasted_iota(jnp.int32, (LOW, 128), 0)
        each = len(flat) // ring * fold
        for group in range(ring // fold):
            stage[...] = jnp.dot(
                jnp.concatenate([r[...] for r in ins[group * each : (group + 1) * each]], axis=1),
                spread_ref[...],
                preferred_element_type=jnp.float32,
            )
            owner = mine + (group * fold + lane // (128 // fold))
            owner = jnp.where(owner >= ring, owner - ring, owner)
            position = owner * all_rows + inside + (first_row + step * tile)

            def one(index, carry):
                held = pl.ds(pl.multiple_of(index * LOW, LOW), LOW)
                error = octet_error(
                    stage[held, i * 128 : (i + 1) * 128] * oct_ref[i : i + 1, :] for i in range(OCTET)
                )
                weight = ((position + index * LOW).astype(jnp.float32) + 0.5) * share + (1.0 / 3.0)
                return carry + error * weight

            sum_ref[...] += lax.fori_loop(0, tile // LOW, one, jnp.zeros((LOW, 128), jnp.float32), unroll=2)

    in_specs = [pl.BlockSpec(memory_space=pltpu.SMEM)]
    for p in flat:
        in_specs.append(pl.BlockSpec((tile, piece), lambda r, o=skip * (p.shape[0] == all_rows): (r + o, 0)))
    in_specs += [
        pl.BlockSpec((OCTET, 128), lambda r: (0, 0)),
        pl.BlockSpec((OCTET * 128, OCTET * 128), lambda r: (0, 0)),
    ]
    return pl.pallas_call(
        kernel,
        grid=(rows // tile,),
        in_specs=in_specs,
        out_specs=pl.BlockSpec((LOW, 128), lambda r: (0, 0)),
        out_shape=jax.ShapeDtypeStruct((LOW, 128), jnp.float32),
        scratch_shapes=[pltpu.VMEM((tile, OCTET * 128), jnp.float32)],
        name="lattice_sum",
    )(place, *flat, scale_own, spread_own)


def mixer_table(mine, ring, blocks):
    side = ring * blocks * LOW
    row = lax.broadcasted_iota(jnp.int32, (side, side), 0)
    col = lax.broadcasted_iota(jnp.int32, (side, side), 1)
    band = blocks * LOW
    first = (((mine + row // band) % ring) * blocks + (row % band) // LOW).astype(jnp.float32)
    second = (((mine - col // band + ring) % ring) * blocks + (col % band) // LOW).astype(jnp.float32)
    order = ring * blocks
    table = math.sqrt(2.0 / order) * jnp.cos(math.pi * (2.0 * second + 1.0) * first / (2.0 * order))
    table = jnp.where(first == 0.0, table * math.sqrt(0.5), table)
    common = (row % LOW) & (col % LOW)
    common = common ^ (common >> 2)
    common = common ^ (common >> 1)
    return jnp.where((common & 1) == 0, table, -table).astype(jnp.bfloat16)


def spread_table(natural, fold):
    side = OCTET * 128
    width = side // fold
    row = lax.broadcasted_iota(jnp.int32, (side, side), 0)
    col = lax.broadcasted_iota(jnp.int32, (side, side), 1)
    column = natural(row % width)
    target = (column % OCTET) * 128 + (row // width) * (width // OCTET) + column // OCTET
    return (target == col).astype(jnp.bfloat16)


def octet_rows(scales):
    turned = jnp.swapaxes(scales.reshape(scales.shape[:-1] + (-1, OCTET)), -1, -2)
    return jnp.concatenate([turned] * (128 // turned.shape[-1]), axis=-1)


def body(weights, left_bits, right_bits, groups):
    experts, local_rows, width = weights.shape
    assert experts == 1
    ring = lax.axis_size("row")
    mine = lax.axis_index("row").astype(jnp.int32)
    blocks_here = local_rows // HB
    chunks = chunk_count(width, ring)
    piece = width // (chunks * ring)
    place = mine.reshape(1)

    def send(x, shift):
        return lax.ppermute(x, "row", [(k, (k + shift) % ring) for k in range(ring)])

    column_args = (weights[0], left_bits, right_bits, place, ring, chunks)
    small, middle = blocks_here // 7, blocks_here * 2 // 7
    thirds = (small, middle, blocks_here - small - middle)
    early, whole, first_row = [], None, 0
    for count in thirds:
        count *= HB
        piece_rows, whole = column_transform(*column_args, first_row, count, math.gcd(first_row, count) or count, whole)
        early.append(piece_rows)
        first_row += count
    splits = (blocks_here // 2, blocks_here - blocks_here // 2)
    step_rows = math.gcd(*(n * HB for n in splits))
    outgoing = [[[rows[s] for rows in early] for s in range(ring)]]
    outgoing += [[[whole[c * ring + s]] for s in range(ring)] for c in range(chunks - 1)]
    mixer = mixer_table(mine, ring, blocks_here)
    band_columns = ring * piece
    spread = spread_table(
        lambda at: (mine - at // piece + ring) % ring * piece + at % piece, OCTET * 128 // band_columns
    )
    spread_own = spread_table(lambda at: at, OCTET * 128 // (chunks * piece))
    own_groups = [
        lax.dynamic_slice_in_dim(groups, (chunk * ring + mine) * piece, piece, 1) for chunk in range(chunks)
    ]
    received, returned, kept = [], [], []
    for chunk in range(chunks):
        leaving = outgoing[chunk][1:]
        if chunk >= AHEAD:
            leaving, received[chunk - AHEAD] = lax.optimization_barrier((leaving, received[chunk - AHEAD]))
        arrived = [[] for _ in range(1, ring)]
        for part in range(len(leaving[0])):
            for s in sorted(range(1, ring), key=lambda s: abs(s - ring // 2)):
                arrived[s - 1].append(send(leaving[s - 1][part], s))
        received.append(arrived)
    peak = jnp.zeros((GROUPS, 128), jnp.float32)
    for chunk in range(chunks):
        last = chunk == chunks - 1
        mixed, peak = row_mix(
            [outgoing[chunk][0]] + received[chunk],
            mixer,
            own_groups[chunk],
            peak,
            splits if last else (blocks_here,),
        )
        if last:
            peaks = [peak] + [send(peak, s) for s in range(1, ring)]
        kept.append(mixed)
        back = []
        for part in range(len(mixed[0])):
            back.append([mixed[0][part]] + [send(mixed[s][part], s) for s in range(1, ring)])
        returned.append(back)

    group_peak = jnp.max(jnp.stack(peaks), axis=(0, 2))
    group_peak = jnp.maximum(group_peak, 1.0)
    in_group = groups == jnp.arange(GROUPS, dtype=jnp.int32)[:, None]
    scale_row = jnp.sum(jnp.where(in_group, (2.0 / group_peak)[:, None], 0.0), axis=0)
    scale_octet = octet_rows(scale_row.reshape(chunks, band_columns)).reshape(chunks * OCTET, 128)
    own_scale = lax.dynamic_slice_in_dim(scale_row.reshape(chunks, ring, piece), mine, 1, 1)
    scale_own = octet_rows(own_scale.reshape(chunks * piece))

    fine = even_tile(step_rows, TILE2)
    ranges = [(sum(splits[:k]) * HB, n * HB) for k, n in enumerate(splits)]
    shares = []
    for part, (first_row, count) in enumerate(ranges):
        own_pieces = [[k[s][part % len(k[s])] for k in kept] for s in range(ring)]
        shares.append(
            lattice_sum(own_pieces, scale_own, spread_own, place, first_row, count, fine, local_rows)
        )
    partial_error = jnp.sum(sum(shares)) / (local_rows * ring * width // OCTET)
    expert_count = lax.axis_size("expert")
    copies = jnp.broadcast_to(partial_error, (expert_count * ring, 1))
    every_error = lax.all_to_all(copies, ("expert", "row"), 0, 0)
    every_error = jnp.sum(every_error.reshape(expert_count, ring), axis=1)
    expert_error = lax.dynamic_slice_in_dim(every_error, lax.axis_index("expert"), 1)
    total_error = jnp.sum(every_error) / expert_count

    before, half_error = (None, None, (local_rows, width)), None
    for chunk in range(chunks):
        back = returned[chunk]
        spans = [(0, local_rows)] if len(back) == 1 else ranges
        given = half_error
        for part, (first_row, count) in enumerate(spans):
            before, half_error = quantize(
                chunk,
                back[part],
                scale_row[None, :],
                scale_octet,
                spread,
                place,
                before,
                given,
                first_row,
                count,
                fine,
            )
    scaled, errors, _ = before
    return (scaled[None], errors[None], (group_peak / 2.0)[None], expert_error, total_error)


def chunk_count(width, ring):
    return min(CHUNKS, width // (128 * ring))


def solution(mesh):
    placed = (P("expert", "row", None), P("expert", "row"), P("expert", None), P("expert", None))
    return jax.shard_map(
        body,
        mesh=mesh,
        in_specs=placed,
        out_specs=(
            P("expert", "row", None),
            P("expert", "row", None),
            P("expert", None),
            P("expert"),
            P(),
        ),
        check_vma=False,
    )
```

```python
import math

import jax
import jax.numpy as jnp
from jax import lax
from jax.experimental import pallas as pl
from jax.experimental.pallas import tpu as pltpu
from jax.sharding import PartitionSpec as P

HB = 128
GROUPS = 16
INNER = 256
LOW = 16
CHUNKS = 4
AHEAD = 3
OCTET = 8
TILE2 = 256


def butterfly(parts):
    parts = list(parts)
    step = 1
    while step < len(parts):
        for base in range(len(parts)):
            if not base & step:
                low, high = parts[base], parts[base | step]
                parts[base], parts[base | step] = low + high, low - high
        step *= 2
    return parts


def even_tile(rows, most):
    return max(t for t in range(HB, most + 1, HB // 2) if rows % t == 0)


def column_transform(weights, left_bits, right_bits, place, ring, chunks, first, rows, tile, before):
    all_rows, width = weights.shape
    skip = first // tile
    count = width // INNER
    piece = width // (chunks * ring)
    root = 1.0 / math.sqrt(width)

    def kernel(place_ref, w_ref, left_ref, right_ref, *rest):
        rest = rest[0 if before is None else len(before) :]
        outs = rest[: chunks * ring]
        table, stage, left_col = rest[chunks * ring :]
        mine = place_ref[0]

        @pl.when(pl.program_id(0) == 0)
        def _():
            common = lax.broadcasted_iota(jnp.int32, (INNER, INNER), 0) & lax.broadcasted_iota(
                jnp.int32, (INNER, INNER), 1
            )
            for bits in (4, 2, 1):
                common = common ^ (common >> bits)
            table[...] = (1 - 2 * (common & 1)).astype(jnp.float32).astype(jnp.bfloat16)

        eye = lax.broadcasted_iota(jnp.int32, (HB, HB), 0) == lax.broadcasted_iota(jnp.int32, (HB, HB), 1)
        for part in range(tile // HB):
            cols = slice(part * HB, (part + 1) * HB)
            signs = (2 * left_ref[:, cols] - 1).astype(jnp.float32) * root
            column = jnp.sum(jnp.where(eye, signs, 0.0), axis=1, keepdims=True)
            left_col[cols, :] = jnp.broadcast_to(column, (HB, INNER))
        right = (2 * right_ref[...] - 1).astype(jnp.float32).astype(jnp.bfloat16)
        signed = [
            w_ref[:, hi * INNER : (hi + 1) * INNER] * right[:, hi * INNER : (hi + 1) * INNER]
            for hi in range(count)
        ]
        turned = jnp.dot(jnp.concatenate(signed, axis=0), table[...], preferred_element_type=jnp.float32)
        stage[...] = turned.reshape(count, tile, INNER)

        def finish(here):
            def one(group, _):
                held = pl.ds(pl.multiple_of(group * LOW, LOW), LOW)
                left = left_col[held, :]
                parts = butterfly([stage[hi, held, :] for hi in range(count)])
                for hi, part in enumerate(parts):
                    part = (part * left).astype(jnp.bfloat16)
                    for begin in range(0, INNER, 128):
                        index, offset = divmod(hi * INNER + begin, piece)
                        chunk, dest = divmod(index, ring)
                        out = outs[chunk * ring + (dest - here) % ring]
                        out[held, offset : offset + 128] = part[:, begin : begin + 128]
                return 0

            lax.fori_loop(0, tile // LOW, one, 0, unroll=2)

        for here in range(ring):
            pl.when(mine == here)(lambda here=here: finish(here))

    pieces = chunks * ring
    operands = [place, weights, left_bits, right_bits]
    in_specs = [
        pl.BlockSpec(memory_space=pltpu.SMEM),
        pl.BlockSpec((tile, width), lambda r: (r + skip, 0)),
        pl.BlockSpec((1, tile), lambda r: (0, r + skip)),
        pl.BlockSpec((1, width), lambda r: (0, 0)),
    ]
    aliases = {}
    if before is not None:
        aliases = {len(operands) + k: ring + k for k in range(len(before))}
        operands += list(before)
        in_specs += [pl.BlockSpec(memory_space=pl.ANY)] * len(before)
    outs = pl.pallas_call(
        kernel,
        grid=(rows // tile,),
        in_specs=in_specs,
        out_specs=[pl.BlockSpec((tile, piece), lambda r: (r, 0))] * ring
        + [pl.BlockSpec((tile, piece), lambda r: (r + skip, 0))] * (pieces - ring),
        out_shape=[jax.ShapeDtypeStruct((rows, piece), jnp.bfloat16)] * ring
        + [jax.ShapeDtypeStruct((all_rows, piece), jnp.bfloat16)] * (pieces - ring),
        scratch_shapes=[
            pltpu.VMEM((INNER, INNER), jnp.bfloat16),
            pltpu.VMEM((count, tile, INNER), jnp.float32),
            pltpu.VMEM((tile, INNER), jnp.float32),
        ],
        input_output_aliases=aliases,
        name="column_transform",
    )(*operands)
    return outs[:ring], outs[ring:]


def row_mix(pieces, mixer, own_groups, before, splits):
    ring = len(pieces)
    width = pieces[0][0].shape[1]
    blocks = sum(splits)
    high = HB // LOW
    band = blocks * LOW
    root = 1.0 / math.sqrt(HB)
    flat = [p.reshape(p.shape[0] // HB, high, LOW, width) for piece in pieces for p in piece]

    def kernel(*refs):
        ins = refs[: len(flat)]
        m_ref, group_ref, before_ref = refs[len(flat) : len(flat) + 3]
        outs, peak_ref, stage = refs[len(flat) + 3 : -2], refs[-2], refs[-1]
        for hi in range(high):
            rhs = jnp.concatenate([r[:, hi].reshape(r.shape[0] * LOW, width) for r in ins], axis=0)
            stage[hi] = jnp.dot(m_ref[...], rhs, preferred_element_type=jnp.float32)

        peak = jnp.zeros((LOW, width), jnp.float32)
        for index, out in enumerate(outs):
            shift, split = divmod(index, len(splits))
            base = shift * band + sum(splits[:split]) * LOW

            def one(a, peak):
                start = pl.multiple_of(base + a * LOW, LOW)
                parts = butterfly([stage[hi, pl.ds(start, LOW), :] for hi in range(high)])
                for hi, part in enumerate(parts):
                    part = part * root
                    peak = jnp.maximum(peak, jnp.abs(part))
                    out[a, hi] = part.astype(jnp.bfloat16)
                return peak

            peak = lax.fori_loop(0, splits[split], one, peak)
        column_peak = jnp.max(peak, axis=0, keepdims=True)
        ids = lax.broadcasted_iota(jnp.int32, (GROUPS, width), 0)
        held = jnp.max(jnp.where(group_ref[...] == ids, column_peak, 0.0), axis=1, keepdims=True)
        peak_ref[...] = jnp.maximum(before_ref[...], held)

    result = pl.pallas_call(
        kernel,
        out_shape=[jax.ShapeDtypeStruct((n, high, LOW, width), jnp.bfloat16) for n in splits] * ring
        + [jax.ShapeDtypeStruct((GROUPS, 128), jnp.float32)],
        scratch_shapes=[pltpu.VMEM((high, ring * band, width), jnp.float32)],
        name="row_mix",
    )(*flat, mixer, own_groups, before)
    mixed = [y.reshape(y.shape[0] * HB, width) for y in result[:-1]]
    return [mixed[s * len(splits) : (s + 1) * len(splits)] for s in range(ring)], result[-1]


def octet_error(values):
    near_sum = low_sum = squares = far_squares = largest = smallest = None
    for value in values:
        near = jnp.floor(value + 0.5)
        low = jnp.floor(value)
        gap = jnp.abs(value - near)
        far = 0.5 - gap
        if near_sum is None:
            near_sum, low_sum, squares, far_squares = near, low, gap * gap, far * far
            largest = smallest = gap
        else:
            near_sum, low_sum = near_sum + near, low_sum + low
            squares, far_squares = squares + gap * gap, far_squares + far * far
            largest, smallest = jnp.maximum(largest, gap), jnp.minimum(smallest, gap)
    near_half, low_half = near_sum * 0.5, low_sum * 0.5
    whole = jnp.where(near_half != jnp.floor(near_half), squares + (1.0 - 2.0 * largest), squares)
    shifted = jnp.where(low_half != jnp.floor(low_half), far_squares + 2.0 * smallest, far_squares)
    return jnp.minimum(whole, shifted)


def quantize(chunk, pieces, scale_row, scale_octet, spread, place, before, halves_error, first_row, rows, tile):
    ring = len(pieces)
    piece = pieces[0].shape[1]
    all_rows, all_width = before[2]
    width = ring * piece
    fold = OCTET * 128 // width
    lanes = width // OCTET
    skip = first_row // tile
    band = tile // fold
    closing = chunk % fold == fold - 1

    def kernel(place_ref, *refs):
        ins = refs[:ring]
        row_ref, oct_ref, spread_ref = refs[ring : ring + 3]
        half_ref = refs[ring + 3] if halves_error is not None else None
        scaled_ref, error_ref, stage = refs[-3:]
        mine = place_ref[0]
        bands = [r[f * band : (f + 1) * band, :] for f in range(fold) for r in ins]
        stage[...] = jnp.dot(
            jnp.concatenate(bands, axis=1), spread_ref[...], preferred_element_type=jnp.float32
        )
        starts = [pl.multiple_of(lax.rem(mine - s + ring, ring) * piece, 128) for s in range(ring)]

        def one(group, _):
            start = pl.multiple_of(group * LOW, LOW)
            for f in range(fold):
                held = pl.ds(f * band + start, LOW)
                for s in range(ring):
                    cols = pl.ds(starts[s], piece)
                    scaled = ins[s][held, :].astype(jnp.float32) * row_ref[:, cols]
                    scaled_ref[held, cols] = scaled.astype(jnp.bfloat16)
            held = pl.ds(start, LOW)
            error = octet_error(stage[held, i * 128 : (i + 1) * 128] * oct_ref[i : i + 1, :] for i in range(OCTET))
            if fold == 1 or not closing:
                error_ref[held, :] = error
            else:
                other = half_ref[held, :]
                left = lax.broadcasted_iota(jnp.int32, (LOW, 128), 1) < lanes
                error_ref[held, :] = jnp.where(left, other, pltpu.roll(error, lanes, 1))
                error_ref[pl.ds(band + start, LOW), :] = jnp.where(left, pltpu.roll(other, lanes, 1), error)
            return 0

        lax.fori_loop(0, band // LOW, one, 0, unroll=True)

    in_specs = [pl.BlockSpec(memory_space=pltpu.SMEM)]
    for p in pieces:
        in_specs.append(pl.BlockSpec((tile, piece), lambda r, o=skip * (p.shape[0] == all_rows): (r + o, 0)))
    in_specs += [
        pl.BlockSpec((1, width), lambda r: (0, chunk)),
        pl.BlockSpec((OCTET, 128), lambda r: (chunk, 0)),
        pl.BlockSpec((OCTET * 128, OCTET * 128), lambda r: (0, 0)),
    ]
    operands = [place, *pieces, scale_row, scale_octet, spread]
    if halves_error is not None:
        in_specs.append(pl.BlockSpec((band, 128), lambda r: (r + skip, 0)))
        operands.append(halves_error)
    aliases = {}
    if before[0] is not None:
        aliases[len(operands)] = 0
        in_specs.append(pl.BlockSpec(memory_space=pl.ANY))
        operands.append(before[0])
    if closing:
        error_spec = pl.BlockSpec((tile, 128), lambda r: (r + skip, chunk // fold))
        error_shape = (all_rows, all_width // OCTET)
        if before[1] is not None:
            aliases[len(operands)] = 1
            in_specs.append(pl.BlockSpec(memory_space=pl.ANY))
            operands.append(before[1])
    else:
        error_spec = pl.BlockSpec((band, 128), lambda r: (r + skip, 0))
        error_shape = (all_rows // fold, 128)
    scaled, errors = pl.pallas_call(
        kernel,
        grid=(rows // tile,),
        in_specs=in_specs,
        out_specs=[pl.BlockSpec((tile, width), lambda r: (r + skip, chunk)), error_spec],
        out_shape=[
            jax.ShapeDtypeStruct((all_rows, all_width), jnp.bfloat16),
            jax.ShapeDtypeStruct(error_shape, jnp.float32),
        ],
        scratch_shapes=[pltpu.VMEM((band, OCTET * 128), jnp.float32)],
        input_output_aliases=aliases,
        name="quantize",
    )(*operands)
    if closing:
        return (scaled, errors, before[2]), None
    return (scaled, before[1], before[2]), errors


def lattice_sum(pieces, scale_own, spread_own, place, first_row, rows, tile, all_rows):
    ring = len(pieces)
    piece = pieces[0][0].shape[1]
    own = len(pieces[0]) * piece
    fold = OCTET * 128 // own
    skip = first_row // tile
    share = 4.0 / (3.0 * all_rows * ring)
    flat = [p for owner in pieces for p in owner]

    def kernel(place_ref, *refs):
        ins, oct_ref, spread_ref, sum_ref, stage = refs[: len(flat)], *refs[len(flat) :]
        mine = place_ref[0]
        step = pl.program_id(0)

        @pl.when(step == 0)
        def _():
            sum_ref[...] = jnp.zeros_like(sum_ref)

        lane = lax.broadcasted_iota(jnp.int32, (LOW, 128), 1)
        inside = lax.broadcasted_iota(jnp.int32, (LOW, 128), 0)
        each = len(flat) // ring * fold
        for group in range(ring // fold):
            stage[...] = jnp.dot(
                jnp.concatenate([r[...] for r in ins[group * each : (group + 1) * each]], axis=1),
                spread_ref[...],
                preferred_element_type=jnp.float32,
            )
            owner = mine + (group * fold + lane // (128 // fold))
            owner = jnp.where(owner >= ring, owner - ring, owner)
            position = owner * all_rows + inside + (first_row + step * tile)

            def one(index, carry):
                held = pl.ds(pl.multiple_of(index * LOW, LOW), LOW)
                error = octet_error(
                    stage[held, i * 128 : (i + 1) * 128] * oct_ref[i : i + 1, :] for i in range(OCTET)
                )
                weight = ((position + index * LOW).astype(jnp.float32) + 0.5) * share + (1.0 / 3.0)
                return carry + error * weight

            sum_ref[...] += lax.fori_loop(0, tile // LOW, one, jnp.zeros((LOW, 128), jnp.float32), unroll=2)

    in_specs = [pl.BlockSpec(memory_space=pltpu.SMEM)]
    for p in flat:
        in_specs.append(pl.BlockSpec((tile, piece), lambda r, o=skip * (p.shape[0] == all_rows): (r + o, 0)))
    in_specs += [
        pl.BlockSpec((OCTET, 128), lambda r: (0, 0)),
        pl.BlockSpec((OCTET * 128, OCTET * 128), lambda r: (0, 0)),
    ]
    return pl.pallas_call(
        kernel,
        grid=(rows // tile,),
        in_specs=in_specs,
        out_specs=pl.BlockSpec((LOW, 128), lambda r: (0, 0)),
        out_shape=jax.ShapeDtypeStruct((LOW, 128), jnp.float32),
        scratch_shapes=[pltpu.VMEM((tile, OCTET * 128), jnp.float32)],
        name="lattice_sum",
    )(place, *flat, scale_own, spread_own)


def mixer_table(mine, ring, blocks):
    side = ring * blocks * LOW
    row = lax.broadcasted_iota(jnp.int32, (side, side), 0)
    col = lax.broadcasted_iota(jnp.int32, (side, side), 1)
    band = blocks * LOW
    first = (((mine + row // band) % ring) * blocks + (row % band) // LOW).astype(jnp.float32)
    second = (((mine - col // band + ring) % ring) * blocks + (col % band) // LOW).astype(jnp.float32)
    order = ring * blocks
    table = math.sqrt(2.0 / order) * jnp.cos(math.pi * (2.0 * second + 1.0) * first / (2.0 * order))
    table = jnp.where(first == 0.0, table * math.sqrt(0.5), table)
    common = (row % LOW) & (col % LOW)
    common = common ^ (common >> 2)
    common = common ^ (common >> 1)
    return jnp.where((common & 1) == 0, table, -table).astype(jnp.bfloat16)


def spread_table(natural, fold):
    side = OCTET * 128
    width = side // fold
    row = lax.broadcasted_iota(jnp.int32, (side, side), 0)
    col = lax.broadcasted_iota(jnp.int32, (side, side), 1)
    column = natural(row % width)
    target = (column % OCTET) * 128 + (row // width) * (width // OCTET) + column // OCTET
    return (target == col).astype(jnp.bfloat16)


def octet_rows(scales):
    turned = jnp.swapaxes(scales.reshape(scales.shape[:-1] + (-1, OCTET)), -1, -2)
    return jnp.concatenate([turned] * (128 // turned.shape[-1]), axis=-1)


def body(weights, left_bits, right_bits, groups):
    experts, local_rows, width = weights.shape
    assert experts == 1
    ring = lax.axis_size("row")
    mine = lax.axis_index("row").astype(jnp.int32)
    blocks_here = local_rows // HB
    chunks = chunk_count(width, ring)
    piece = width // (chunks * ring)
    place = mine.reshape(1)

    def send(x, shift):
        return lax.ppermute(x, "row", [(k, (k + shift) % ring) for k in range(ring)])

    column_args = (weights[0], left_bits, right_bits, place, ring, chunks)
    small, middle = blocks_here // 7, blocks_here * 2 // 7
    thirds = (small, middle, blocks_here - small - middle)
    early, whole, first_row = [], None, 0
    for count in thirds:
        count *= HB
        piece_rows, whole = column_transform(*column_args, first_row, count, math.gcd(first_row, count) or count, whole)
        early.append(piece_rows)
        first_row += count
    splits = thirds[::-1]
    step_rows = math.gcd(*(n * HB for n in splits))
    outgoing = [[[rows[s] for rows in early] for s in range(ring)]]
    outgoing += [[[whole[c * ring + s]] for s in range(ring)] for c in range(chunks - 1)]
    mixer = mixer_table(mine, ring, blocks_here)
    band_columns = ring * piece
    spread = spread_table(
        lambda at: (mine - at // piece + ring) % ring * piece + at % piece, OCTET * 128 // band_columns
    )
    spread_own = spread_table(lambda at: at, OCTET * 128 // (chunks * piece))
    own_groups = [
        lax.dynamic_slice_in_dim(groups, (chunk * ring + mine) * piece, piece, 1) for chunk in range(chunks)
    ]
    received, returned, kept = [], [], []
    for chunk in range(chunks):
        leaving = outgoing[chunk][1:]
        if chunk >= AHEAD:
            leaving, received[chunk - AHEAD] = lax.optimization_barrier((leaving, received[chunk - AHEAD]))
        arrived = [[] for _ in range(1, ring)]
        for part in range(len(leaving[0])):
            for s in sorted(range(1, ring), key=lambda s: abs(s - ring // 2)):
                arrived[s - 1].append(send(leaving[s - 1][part], s))
        received.append(arrived)
    peak = jnp.zeros((GROUPS, 128), jnp.float32)
    for chunk in range(chunks):
        last = chunk == chunks - 1
        mixed, peak = row_mix(
            [outgoing[chunk][0]] + received[chunk],
            mixer,
            own_groups[chunk],
            peak,
            splits if last else (blocks_here,),
        )
        if last:
            peaks = [peak] + [send(peak, s) for s in range(1, ring)]
        kept.append(mixed)
        back = []
        for part in range(len(mixed[0])):
            back.append([mixed[0][part]] + [send(mixed[s][part], s) for s in range(1, ring)])
        returned.append(back)

    group_peak = jnp.max(jnp.stack(peaks), axis=(0, 2))
    group_peak = jnp.maximum(group_peak, 1.0)
    in_group = groups == jnp.arange(GROUPS, dtype=jnp.int32)[:, None]
    scale_row = jnp.sum(jnp.where(in_group, (2.0 / group_peak)[:, None], 0.0), axis=0)
    scale_octet = octet_rows(scale_row.reshape(chunks, band_columns)).reshape(chunks * OCTET, 128)
    own_scale = lax.dynamic_slice_in_dim(scale_row.reshape(chunks, ring, piece), mine, 1, 1)
    scale_own = octet_rows(own_scale.reshape(chunks * piece))

    fine = even_tile(step_rows, TILE2)
    ranges = [(sum(splits[:k]) * HB, n * HB) for k, n in enumerate(splits)]
    shares = []
    for part, (first_row, count) in enumerate(ranges):
        own_pieces = [[k[s][part % len(k[s])] for k in kept] for s in range(ring)]
        shares.append(
            lattice_sum(own_pieces, scale_own, spread_own, place, first_row, count, fine, local_rows)
        )
    partial_error = jnp.sum(sum(shares)) / (local_rows * ring * width // OCTET)
    expert_count = lax.axis_size("expert")
    copies = jnp.broadcast_to(partial_error, (expert_count * ring, 1))
    every_error = lax.all_to_all(copies, ("expert", "row"), 0, 0)
    every_error = jnp.sum(every_error.reshape(expert_count, ring), axis=1)
    expert_error = lax.dynamic_slice_in_dim(every_error, lax.axis_index("expert"), 1)
    total_error = jnp.sum(every_error) / expert_count

    before, half_error = (None, None, (local_rows, width)), None
    for chunk in range(chunks):
        back = returned[chunk]
        spans = [(0, local_rows)] if len(back) == 1 else ranges
        given = half_error
        for part, (first_row, count) in enumerate(spans):
            before, half_error = quantize(
                chunk,
                back[part],
                scale_row[None, :],
                scale_octet,
                spread,
                place,
                before,
                given,
                first_row,
                count,
                fine,
            )
    scaled, errors, _ = before
    return (scaled[None], errors[None], (group_peak / 2.0)[None], expert_error, total_error)


def chunk_count(width, ring):
    return min(CHUNKS, width // (128 * ring))


def solution(mesh):
    placed = (P("expert", "row", None), P("expert", "row"), P("expert", None), P("expert", None))
    return jax.shard_map(
        body,
        mesh=mesh,
        in_specs=placed,
        out_specs=(
            P("expert", "row", None),
            P("expert", "row", None),
            P("expert", None),
            P("expert"),
            P(),
        ),
        check_vma=False,
    )
```

```python
import math

import jax
import jax.numpy as jnp
from jax import lax
from jax.experimental import pallas as pl
from jax.experimental.pallas import tpu as pltpu
from jax.sharding import PartitionSpec as P

HB = 128
GROUPS = 16
INNER = 256
LOW = 16
CHUNKS = 4
AHEAD = 3
OCTET = 8
TILE2 = 448


def butterfly(parts):
    parts = list(parts)
    step = 1
    while step < len(parts):
        for base in range(len(parts)):
            if not base & step:
                low, high = parts[base], parts[base | step]
                parts[base], parts[base | step] = low + high, low - high
        step *= 2
    return parts


def even_tile(rows, most):
    return max(t for t in range(HB, most + 1, HB // 2) if rows % t == 0)


def column_transform(weights, left_bits, right_bits, place, ring, chunks, first, rows, tile, before):
    all_rows, width = weights.shape
    skip = first // tile
    count = width // INNER
    piece = width // (chunks * ring)
    root = 1.0 / math.sqrt(width)

    def kernel(place_ref, w_ref, left_ref, right_ref, *rest):
        rest = rest[0 if before is None else len(before) :]
        outs = rest[: chunks * ring]
        table, stage, left_col = rest[chunks * ring :]
        mine = place_ref[0]

        @pl.when(pl.program_id(0) == 0)
        def _():
            common = lax.broadcasted_iota(jnp.int32, (INNER, INNER), 0) & lax.broadcasted_iota(
                jnp.int32, (INNER, INNER), 1
            )
            for bits in (4, 2, 1):
                common = common ^ (common >> bits)
            table[...] = (1 - 2 * (common & 1)).astype(jnp.float32).astype(jnp.bfloat16)

        eye = lax.broadcasted_iota(jnp.int32, (HB, HB), 0) == lax.broadcasted_iota(jnp.int32, (HB, HB), 1)
        for part in range(tile // HB):
            cols = slice(part * HB, (part + 1) * HB)
            signs = (2 * left_ref[:, cols] - 1).astype(jnp.float32) * root
            column = jnp.sum(jnp.where(eye, signs, 0.0), axis=1, keepdims=True)
            left_col[cols, :] = jnp.broadcast_to(column, (HB, INNER))
        right = (2 * right_ref[...] - 1).astype(jnp.float32).astype(jnp.bfloat16)
        signed = [
            w_ref[:, hi * INNER : (hi + 1) * INNER] * right[:, hi * INNER : (hi + 1) * INNER]
            for hi in range(count)
        ]
        turned = jnp.dot(jnp.concatenate(signed, axis=0), table[...], preferred_element_type=jnp.float32)
        stage[...] = turned.reshape(count, tile, INNER)

        def finish(here):
            def one(group, _):
                held = pl.ds(pl.multiple_of(group * LOW, LOW), LOW)
                left = left_col[held, :]
                parts = butterfly([stage[hi, held, :] for hi in range(count)])
                for hi, part in enumerate(parts):
                    part = (part * left).astype(jnp.bfloat16)
                    for begin in range(0, INNER, 128):
                        index, offset = divmod(hi * INNER + begin, piece)
                        chunk, dest = divmod(index, ring)
                        out = outs[chunk * ring + (dest - here) % ring]
                        out[held, offset : offset + 128] = part[:, begin : begin + 128]
                return 0

            lax.fori_loop(0, tile // LOW, one, 0, unroll=2)

        for here in range(ring):
            pl.when(mine == here)(lambda here=here: finish(here))

    pieces = chunks * ring
    operands = [place, weights, left_bits, right_bits]
    in_specs = [
        pl.BlockSpec(memory_space=pltpu.SMEM),
        pl.BlockSpec((tile, width), lambda r: (r + skip, 0)),
        pl.BlockSpec((1, tile), lambda r: (0, r + skip)),
        pl.BlockSpec((1, width), lambda r: (0, 0)),
    ]
    aliases = {}
    if before is not None:
        aliases = {len(operands) + k: ring + k for k in range(len(before))}
        operands += list(before)
        in_specs += [pl.BlockSpec(memory_space=pl.ANY)] * len(before)
    outs = pl.pallas_call(
        kernel,
        grid=(rows // tile,),
        in_specs=in_specs,
        out_specs=[pl.BlockSpec((tile, piece), lambda r: (r, 0))] * ring
        + [pl.BlockSpec((tile, piece), lambda r: (r + skip, 0))] * (pieces - ring),
        out_shape=[jax.ShapeDtypeStruct((rows, piece), jnp.bfloat16)] * ring
        + [jax.ShapeDtypeStruct((all_rows, piece), jnp.bfloat16)] * (pieces - ring),
        scratch_shapes=[
            pltpu.VMEM((INNER, INNER), jnp.bfloat16),
            pltpu.VMEM((count, tile, INNER), jnp.float32),
            pltpu.VMEM((tile, INNER), jnp.float32),
        ],
        input_output_aliases=aliases,
        name="column_transform",
    )(*operands)
    return outs[:ring], outs[ring:]


def row_mix(pieces, mixer, own_groups, before, splits):
    ring = len(pieces)
    width = pieces[0][0].shape[1]
    blocks = sum(splits)
    high = HB // LOW
    band = blocks * LOW
    root = 1.0 / math.sqrt(HB)
    flat = [p.reshape(p.shape[0] // HB, high, LOW, width) for piece in pieces for p in piece]

    def kernel(*refs):
        ins = refs[: len(flat)]
        m_ref, group_ref, before_ref = refs[len(flat) : len(flat) + 3]
        outs, peak_ref, stage = refs[len(flat) + 3 : -2], refs[-2], refs[-1]
        for hi in range(high):
            rhs = jnp.concatenate([r[:, hi].reshape(r.shape[0] * LOW, width) for r in ins], axis=0)
            stage[hi] = jnp.dot(m_ref[...], rhs, preferred_element_type=jnp.float32)

        peak = jnp.zeros((LOW, width), jnp.float32)
        for index, out in enumerate(outs):
            shift, split = divmod(index, len(splits))
            base = shift * band + sum(splits[:split]) * LOW

            def one(a, peak):
                start = pl.multiple_of(base + a * LOW, LOW)
                parts = butterfly([stage[hi, pl.ds(start, LOW), :] for hi in range(high)])
                for hi, part in enumerate(parts):
                    part = part * root
                    peak = jnp.maximum(peak, jnp.abs(part))
                    out[a, hi] = part.astype(jnp.bfloat16)
                return peak

            peak = lax.fori_loop(0, splits[split], one, peak)
        column_peak = jnp.max(peak, axis=0, keepdims=True)
        ids = lax.broadcasted_iota(jnp.int32, (GROUPS, width), 0)
        held = jnp.max(jnp.where(group_ref[...] == ids, column_peak, 0.0), axis=1, keepdims=True)
        peak_ref[...] = jnp.maximum(before_ref[...], held)

    result = pl.pallas_call(
        kernel,
        out_shape=[jax.ShapeDtypeStruct((n, high, LOW, width), jnp.bfloat16) for n in splits] * ring
        + [jax.ShapeDtypeStruct((GROUPS, 128), jnp.float32)],
        scratch_shapes=[pltpu.VMEM((high, ring * band, width), jnp.float32)],
        name="row_mix",
    )(*flat, mixer, own_groups, before)
    mixed = [y.reshape(y.shape[0] * HB, width) for y in result[:-1]]
    return [mixed[s * len(splits) : (s + 1) * len(splits)] for s in range(ring)], result[-1]


def octet_error(values):
    near_sum = low_sum = squares = far_squares = largest = smallest = None
    for value in values:
        near = jnp.floor(value + 0.5)
        low = jnp.floor(value)
        gap = jnp.abs(value - near)
        far = 0.5 - gap
        if near_sum is None:
            near_sum, low_sum, squares, far_squares = near, low, gap * gap, far * far
            largest = smallest = gap
        else:
            near_sum, low_sum = near_sum + near, low_sum + low
            squares, far_squares = squares + gap * gap, far_squares + far * far
            largest, smallest = jnp.maximum(largest, gap), jnp.minimum(smallest, gap)
    near_half, low_half = near_sum * 0.5, low_sum * 0.5
    whole = jnp.where(near_half != jnp.floor(near_half), squares + (1.0 - 2.0 * largest), squares)
    shifted = jnp.where(low_half != jnp.floor(low_half), far_squares + 2.0 * smallest, far_squares)
    return jnp.minimum(whole, shifted)


def quantize(chunk, pieces, scale_row, scale_octet, spread, place, before, halves_error, first_row, rows, tile):
    ring = len(pieces)
    piece = pieces[0].shape[1]
    all_rows, all_width = before[2]
    width = ring * piece
    fold = OCTET * 128 // width
    lanes = width // OCTET
    skip = first_row // tile
    band = tile // fold
    closing = chunk % fold == fold - 1

    def kernel(place_ref, *refs):
        ins = refs[:ring]
        row_ref, oct_ref, spread_ref = refs[ring : ring + 3]
        half_ref = refs[ring + 3] if halves_error is not None else None
        scaled_ref, error_ref, stage = refs[-3:]
        mine = place_ref[0]
        bands = [r[f * band : (f + 1) * band, :] for f in range(fold) for r in ins]
        stage[...] = jnp.dot(
            jnp.concatenate(bands, axis=1), spread_ref[...], preferred_element_type=jnp.float32
        )
        starts = [pl.multiple_of(lax.rem(mine - s + ring, ring) * piece, 128) for s in range(ring)]

        def one(group, _):
            start = pl.multiple_of(group * LOW, LOW)
            for f in range(fold):
                held = pl.ds(f * band + start, LOW)
                for s in range(ring):
                    cols = pl.ds(starts[s], piece)
                    scaled = ins[s][held, :].astype(jnp.float32) * row_ref[:, cols]
                    scaled_ref[held, cols] = scaled.astype(jnp.bfloat16)
            held = pl.ds(start, LOW)
            error = octet_error(stage[held, i * 128 : (i + 1) * 128] * oct_ref[i : i + 1, :] for i in range(OCTET))
            if fold == 1 or not closing:
                error_ref[held, :] = error
            else:
                other = half_ref[held, :]
                left = lax.broadcasted_iota(jnp.int32, (LOW, 128), 1) < lanes
                error_ref[held, :] = jnp.where(left, other, pltpu.roll(error, lanes, 1))
                error_ref[pl.ds(band + start, LOW), :] = jnp.where(left, pltpu.roll(other, lanes, 1), error)
            return 0

        lax.fori_loop(0, band // LOW, one, 0, unroll=True)

    in_specs = [pl.BlockSpec(memory_space=pltpu.SMEM)]
    for p in pieces:
        in_specs.append(pl.BlockSpec((tile, piece), lambda r, o=skip * (p.shape[0] == all_rows): (r + o, 0)))
    in_specs += [
        pl.BlockSpec((1, width), lambda r: (0, chunk)),
        pl.BlockSpec((OCTET, 128), lambda r: (chunk, 0)),
        pl.BlockSpec((OCTET * 128, OCTET * 128), lambda r: (0, 0)),
    ]
    operands = [place, *pieces, scale_row, scale_octet, spread]
    if halves_error is not None:
        in_specs.append(pl.BlockSpec((band, 128), lambda r: (r + skip, 0)))
        operands.append(halves_error)
    aliases = {}
    if before[0] is not None:
        aliases[len(operands)] = 0
        in_specs.append(pl.BlockSpec(memory_space=pl.ANY))
        operands.append(before[0])
    if closing:
        error_spec = pl.BlockSpec((tile, 128), lambda r: (r + skip, chunk // fold))
        error_shape = (all_rows, all_width // OCTET)
        if before[1] is not None:
            aliases[len(operands)] = 1
            in_specs.append(pl.BlockSpec(memory_space=pl.ANY))
            operands.append(before[1])
    else:
        error_spec = pl.BlockSpec((band, 128), lambda r: (r + skip, 0))
        error_shape = (all_rows // fold, 128)
    scaled, errors = pl.pallas_call(
        kernel,
        grid=(rows // tile,),
        in_specs=in_specs,
        out_specs=[pl.BlockSpec((tile, width), lambda r: (r + skip, chunk)), error_spec],
        out_shape=[
            jax.ShapeDtypeStruct((all_rows, all_width), jnp.bfloat16),
            jax.ShapeDtypeStruct(error_shape, jnp.float32),
        ],
        scratch_shapes=[pltpu.VMEM((band, OCTET * 128), jnp.float32)],
        input_output_aliases=aliases,
        name="quantize",
    )(*operands)
    if closing:
        return (scaled, errors, before[2]), None
    return (scaled, before[1], before[2]), errors


def lattice_sum(pieces, scale_own, spread_own, place, first_row, rows, tile, all_rows):
    ring = len(pieces)
    piece = pieces[0][0].shape[1]
    own = len(pieces[0]) * piece
    fold = OCTET * 128 // own
    skip = first_row // tile
    share = 4.0 / (3.0 * all_rows * ring)
    flat = [p for owner in pieces for p in owner]

    def kernel(place_ref, *refs):
        ins, oct_ref, spread_ref, sum_ref, stage = refs[: len(flat)], *refs[len(flat) :]
        mine = place_ref[0]
        step = pl.program_id(0)

        @pl.when(step == 0)
        def _():
            sum_ref[...] = jnp.zeros_like(sum_ref)

        lane = lax.broadcasted_iota(jnp.int32, (LOW, 128), 1)
        inside = lax.broadcasted_iota(jnp.int32, (LOW, 128), 0)
        each = len(flat) // ring * fold
        for group in range(ring // fold):
            stage[...] = jnp.dot(
                jnp.concatenate([r[...] for r in ins[group * each : (group + 1) * each]], axis=1),
                spread_ref[...],
                preferred_element_type=jnp.float32,
            )
            owner = mine + (group * fold + lane // (128 // fold))
            owner = jnp.where(owner >= ring, owner - ring, owner)
            position = owner * all_rows + inside + (first_row + step * tile)

            def one(index, carry):
                held = pl.ds(pl.multiple_of(index * LOW, LOW), LOW)
                error = octet_error(
                    stage[held, i * 128 : (i + 1) * 128] * oct_ref[i : i + 1, :] for i in range(OCTET)
                )
                weight = ((position + index * LOW).astype(jnp.float32) + 0.5) * share + (1.0 / 3.0)
                return carry + error * weight

            sum_ref[...] += lax.fori_loop(0, tile // LOW, one, jnp.zeros((LOW, 128), jnp.float32), unroll=2)

    in_specs = [pl.BlockSpec(memory_space=pltpu.SMEM)]
    for p in flat:
        in_specs.append(pl.BlockSpec((tile, piece), lambda r, o=skip * (p.shape[0] == all_rows): (r + o, 0)))
    in_specs += [
        pl.BlockSpec((OCTET, 128), lambda r: (0, 0)),
        pl.BlockSpec((OCTET * 128, OCTET * 128), lambda r: (0, 0)),
    ]
    return pl.pallas_call(
        kernel,
        grid=(rows // tile,),
        in_specs=in_specs,
        out_specs=pl.BlockSpec((LOW, 128), lambda r: (0, 0)),
        out_shape=jax.ShapeDtypeStruct((LOW, 128), jnp.float32),
        scratch_shapes=[pltpu.VMEM((tile, OCTET * 128), jnp.float32)],
        name="lattice_sum",
    )(place, *flat, scale_own, spread_own)


def mixer_table(mine, ring, blocks):
    side = ring * blocks * LOW
    row = lax.broadcasted_iota(jnp.int32, (side, side), 0)
    col = lax.broadcasted_iota(jnp.int32, (side, side), 1)
    band = blocks * LOW
    first = (((mine + row // band) % ring) * blocks + (row % band) // LOW).astype(jnp.float32)
    second = (((mine - col // band + ring) % ring) * blocks + (col % band) // LOW).astype(jnp.float32)
    order = ring * blocks
    table = math.sqrt(2.0 / order) * jnp.cos(math.pi * (2.0 * second + 1.0) * first / (2.0 * order))
    table = jnp.where(first == 0.0, table * math.sqrt(0.5), table)
    common = (row % LOW) & (col % LOW)
    common = common ^ (common >> 2)
    common = common ^ (common >> 1)
    return jnp.where((common & 1) == 0, table, -table).astype(jnp.bfloat16)


def spread_table(natural, fold):
    side = OCTET * 128
    width = side // fold
    row = lax.broadcasted_iota(jnp.int32, (side, side), 0)
    col = lax.broadcasted_iota(jnp.int32, (side, side), 1)
    column = natural(row % width)
    target = (column % OCTET) * 128 + (row // width) * (width // OCTET) + column // OCTET
    return (target == col).astype(jnp.bfloat16)


def octet_rows(scales):
    turned = jnp.swapaxes(scales.reshape(scales.shape[:-1] + (-1, OCTET)), -1, -2)
    return jnp.concatenate([turned] * (128 // turned.shape[-1]), axis=-1)


def body(weights, left_bits, right_bits, groups):
    experts, local_rows, width = weights.shape
    assert experts == 1
    ring = lax.axis_size("row")
    mine = lax.axis_index("row").astype(jnp.int32)
    blocks_here = local_rows // HB
    chunks = chunk_count(width, ring)
    piece = width // (chunks * ring)
    place = mine.reshape(1)

    def send(x, shift):
        return lax.ppermute(x, "row", [(k, (k + shift) % ring) for k in range(ring)])

    column_args = (weights[0], left_bits, right_bits, place, ring, chunks)
    small = max(blocks_here * 2 // 7, 1)
    parts = (small, blocks_here - small)
    early, whole, first_row = [], None, 0
    for count in parts:
        count *= HB
        piece_rows, whole = column_transform(*column_args, first_row, count, math.gcd(first_row, count) or count, whole)
        early.append(piece_rows)
        first_row += count
    splits = (blocks_here // 2, blocks_here - blocks_here // 2)
    step_rows = math.gcd(*(n * HB for n in splits))
    outgoing = [[[rows[s] for rows in early] for s in range(ring)]]
    outgoing += [[[whole[c * ring + s]] for s in range(ring)] for c in range(chunks - 1)]
    mixer = mixer_table(mine, ring, blocks_here)
    band_columns = ring * piece
    spread = spread_table(
        lambda at: (mine - at // piece + ring) % ring * piece + at % piece, OCTET * 128 // band_columns
    )
    spread_own = spread_table(lambda at: at, OCTET * 128 // (chunks * piece))
    own_groups = [
        lax.dynamic_slice_in_dim(groups, (chunk * ring + mine) * piece, piece, 1) for chunk in range(chunks)
    ]
    received, returned, kept = [], [], []
    for chunk in range(chunks):
        leaving = outgoing[chunk][1:]
        if chunk >= AHEAD:
            leaving, received[chunk - AHEAD] = lax.optimization_barrier((leaving, received[chunk - AHEAD]))
        arrived = [[] for _ in range(1, ring)]
        for part in range(len(leaving[0])):
            for s in sorted(range(1, ring), key=lambda s: abs(s - ring // 2)):
                arrived[s - 1].append(send(leaving[s - 1][part], s))
        received.append(arrived)
    peak = jnp.zeros((GROUPS, 128), jnp.float32)
    for chunk in range(chunks):
        last = chunk == chunks - 1
        mixed, peak = row_mix(
            [outgoing[chunk][0]] + received[chunk],
            mixer,
            own_groups[chunk],
            peak,
            splits if last else (blocks_here,),
        )
        if last:
            peaks = [peak] + [send(peak, s) for s in range(1, ring)]
        kept.append(mixed)
        back = []
        for part in range(len(mixed[0])):
            back.append([mixed[0][part]] + [send(mixed[s][part], s) for s in range(1, ring)])
        returned.append(back)

    group_peak = jnp.max(jnp.stack(peaks), axis=(0, 2))
    group_peak = jnp.maximum(group_peak, 1.0)
    in_group = groups == jnp.arange(GROUPS, dtype=jnp.int32)[:, None]
    scale_row = jnp.sum(jnp.where(in_group, (2.0 / group_peak)[:, None], 0.0), axis=0)
    scale_octet = octet_rows(scale_row.reshape(chunks, band_columns)).reshape(chunks * OCTET, 128)
    own_scale = lax.dynamic_slice_in_dim(scale_row.reshape(chunks, ring, piece), mine, 1, 1)
    scale_own = octet_rows(own_scale.reshape(chunks * piece))

    fine = even_tile(step_rows, TILE2)
    ranges = [(sum(splits[:k]) * HB, n * HB) for k, n in enumerate(splits)]
    shares = []
    for part, (first_row, count) in enumerate(ranges):
        own_pieces = [[k[s][part % len(k[s])] for k in kept] for s in range(ring)]
        shares.append(
            lattice_sum(own_pieces, scale_own, spread_own, place, first_row, count, fine, local_rows)
        )
    partial_error = jnp.sum(sum(shares)) / (local_rows * ring * width // OCTET)
    expert_count = lax.axis_size("expert")
    copies = jnp.broadcast_to(partial_error, (expert_count * ring, 1))
    every_error = lax.all_to_all(copies, ("expert", "row"), 0, 0)
    every_error = jnp.sum(every_error.reshape(expert_count, ring), axis=1)
    expert_error = lax.dynamic_slice_in_dim(every_error, lax.axis_index("expert"), 1)
    total_error = jnp.sum(every_error) / expert_count

    before, half_error = (None, None, (local_rows, width)), None
    for chunk in range(chunks):
        back = returned[chunk]
        spans = [(0, local_rows)] if len(back) == 1 else ranges
        given = half_error
        for part, (first_row, count) in enumerate(spans):
            before, half_error = quantize(
                chunk,
                back[part],
                scale_row[None, :],
                scale_octet,
                spread,
                place,
                before,
                given,
                first_row,
                count,
                fine,
            )
    scaled, errors, _ = before
    return (scaled[None], errors[None], (group_peak / 2.0)[None], expert_error, total_error)


def chunk_count(width, ring):
    return min(CHUNKS, width // (128 * ring))


def solution(mesh):
    placed = (P("expert", "row", None), P("expert", "row"), P("expert", None), P("expert", None))
    return jax.shard_map(
        body,
        mesh=mesh,
        in_specs=placed,
        out_specs=(
            P("expert", "row", None),
            P("expert", "row", None),
            P("expert", None),
            P("expert"),
            P(),
        ),
        check_vma=False,
    )
```
